32 devices in a mesh: member: 2 (over y), gx: 4 (over z), gy: 4 (over x, core).
Axes of the slice: x: 2, y: 2, z: 4, core: 2. Of those that a mesh axis runs over, the one named last changes fastest.
Arguments:
- populations: float32 [19, 32, 64, 128], P(None, ('member', 'gx'), 'gy'), parts along dimension 1, may hold values from 0 to 1, as said below
- heat_level: int32 [32, 64, 128], P(('member', 'gx'), 'gy'), parts along dimension 0, may hold values from 0 to 7
- obstacle: int32 [32, 64, 128], P(('member', 'gx'), 'gy'), parts along dimension 0, may hold values 0 or 1
- heat_table: float32 [8], replicated, may hold values from 0.02 to 0.5
Outputs:
- final_populations: float32 [19, 32, 64, 128], P(None, ('member', 'gx'), 'gy'), parts along dimension 1
- velocity: float32 [3, 32, 64, 128], P(None, ('member', 'gx'), 'gy'), parts along dimension 1
The draws below stay inside these ranges and needn't reach their ends.
There are 2 independent parts, one for each index of `member`. The reference program is written for one: setup_inputs(seed, part) draws one part's arguments, and reference() takes and returns one part's arrays. A program takes and returns all parts, laid end to end along the dimension named above; an argument that names none is the same for every part. Nothing has to cross between parts.
Inputs may be any that keep to these rules, and one draw needn't show every extreme that they name: Positive populations near a local equilibrium, in the direction order of the steps.
All inputs are finite; a program needn't handle non-finite values. No bound on the sum of `obstacle` on one device may be relied on, other than what follows from the above.
Results may differ from the reference program's by a relative error of at most 0.0001.
Values sent between devices are 32-bit elements; how exact they have to be, the bound alone decides.
No kernel may reach another device: no remote copies, remote signals or barrier semaphores. Data moves between devices by JAX's collectives and lax.ppermute only.
A program may use at most 64 MiB of HBM per device.

```python
import math
import jax
import jax.numpy as jnp
import numpy as np
from jax import lax

NZ = 128
STEPS = 2
LEVELS = 8
NX = 16
NY = 64


lattice = np.array([[0, 0, 0], [1, 0, 0], [-1, 0, 0], [0, 1, 0], [0, -1, 0], [0, 0, 1], [0, 0, -1], [1, 1, 0], [-1, -1, 0], [1, -1, 0], [-1, 1, 0], [1, 0, 1], [-1, 0, -1], [1, 0, -1], [-1, 0, 1], [0, 1, 1], [0, -1, -1], [0, 1, -1], [0, -1, 1]])


lattice_weight = [1.0 / 3.0] + [1.0 / 18.0] * 6 + [1.0 / 36.0] * 12


def draw_populations(key, part):
    key_one, key_two, key_three, key_four, key_five, key_six, key_seven = jax.random.split(jax.random.fold_in(key, 11), 7)
    grid_x = lax.broadcasted_iota(jnp.float32, (NX, NY, NZ), 0)
    grid_y = lax.broadcasted_iota(jnp.float32, (NX, NY, NZ), 1)
    amplitude = jnp.exp(jax.random.uniform(key_four, (), jnp.float32, math.log(0.01), math.log(0.03)))
    speed_ramp = amplitude * (1.0 + grid_x / NX + grid_y / NY)
    sample = jnp.clip(jax.random.normal(key_one, (3, NX, NY, NZ), jnp.float32), -2.5, 2.5)
    density = 1.0 + jax.random.uniform(key_two, (NX, NY, NZ), jnp.float32, -0.05, 0.05)
    velocity = sample * speed_ramp[None]
    plant_speed = jax.random.uniform(key_five, (), jnp.float32, 0.15, 0.4)
    plant_angle = jax.random.uniform(key_six, (), jnp.float32, -math.pi, math.pi)
    key_cx, key_cy, key_cz = jax.random.split(key_seven, 3)
    centre_x = jax.random.randint(key_cx, (), 2, NX - 2)
    centre_y = jax.random.randint(key_cy, (), 3, NY - 3)
    centre_z = jax.random.randint(key_cz, (), 3, NZ - 3)
    index_x = lax.broadcasted_iota(jnp.int32, (NX, NY, NZ), 0)
    index_y = lax.broadcasted_iota(jnp.int32, (NX, NY, NZ), 1)
    index_z = lax.broadcasted_iota(jnp.int32, (NX, NY, NZ), 2)
    region = (jnp.abs(index_x - centre_x) <= 2) & (jnp.abs(index_y - centre_y) <= 2) & (jnp.abs(index_z - centre_z) <= 2)
    planted = plant_speed * jnp.stack([0.9 * jnp.cos(plant_angle), 0.9 * jnp.sin(plant_angle), jnp.float32(0.436)])
    velocity = jnp.where(region[None], planted[:, None, None, None], velocity)
    jitter = jnp.clip(jax.random.normal(key_three, (19, NX, NY, NZ), jnp.float32), -3.0, 3.0)
    speed_sq = velocity[0] * velocity[0] + velocity[1] * velocity[1] + velocity[2] * velocity[2]
    pieces = []
    for number in range(19):
        project = float(lattice[number][0]) * velocity[0] + float(lattice[number][1]) * velocity[1] + float(lattice[number][2]) * velocity[2]
        equilibrium = lattice_weight[number] * density * (1.0 + 3.0 * project + 4.5 * project * project - 1.5 * speed_sq)
        pieces.append(equilibrium * (1.0 + 0.05 * jitter[number]))
    return jnp.stack(pieces).astype(jnp.float32)


def with_ends(values, own_key, least, top_value):
    index_at = [jax.random.randint(jax.random.fold_in(own_key, axis), (), 0, length) for axis, length in enumerate(values.shape)]
    main_axis = values.shape.index(max(values.shape))
    next_to = index_at[:main_axis] + [(index_at[main_axis] + 1) % values.shape[main_axis]] + index_at[main_axis + 1:]
    return values.at[tuple(index_at)].set(least).at[tuple(next_to)].set(top_value)


def setup_inputs(seed: int = 0, part: int = 0) -> dict:
    key_of = jax.random.split(jax.random.key(seed), 5)
    own_keys = jax.random.split(jax.random.fold_in(key_of[4], part), 5)
    populations = draw_populations(jax.random.fold_in(jax.random.fold_in(key_of[4], part), 71), part)
    heat_level = with_ends(jax.random.randint(own_keys[1], (NX, NY, NZ), 0, LEVELS), jax.random.fold_in(own_keys[1], 1), 0, LEVELS - 1).astype(jnp.int32)
    obstacle = with_ends((jax.random.randint(own_keys[2], (NX, NY, NZ), 0, 10) < 1).astype(jnp.int32), jax.random.fold_in(own_keys[2], 1), 0, 1)
    heat_table = jnp.clip(jnp.exp(jax.random.uniform(key_of[3], (LEVELS,), jnp.float32, math.log(0.02), math.log(0.5))), 0.02, 0.5)
    return {"populations": populations, "heat_level": heat_level, "obstacle": obstacle, "heat_table": heat_table}


lattice = np.array([[0, 0, 0], [1, 0, 0], [-1, 0, 0], [0, 1, 0], [0, -1, 0], [0, 0, 1], [0, 0, -1], [1, 1, 0], [-1, -1, 0], [1, -1, 0], [-1, 1, 0], [1, 0, 1], [-1, 0, -1], [1, 0, -1], [-1, 0, 1], [0, 1, 1], [0, -1, -1], [0, 1, -1], [0, -1, 1]])
lattice_weight = [1.0 / 3.0] + [1.0 / 18.0] * 6 + [1.0 / 36.0] * 12
opposite = [0, 2, 1, 4, 3, 6, 5, 8, 7, 10, 9, 12, 11, 14, 13, 16, 15, 18, 17]
base_tau = 0.52
smag_coef = 0.04
speed_cap = 0.1
strain_floor = 1e-06

def stream_all(padded, span_x, span_y, depth_z):
    pieces = []
    for number in range(19):
        shift_x = int(lattice[number][0])
        shift_y = int(lattice[number][1])
        shift_z = int(lattice[number][2])
        pieces.append(padded[number, 1 - shift_x:1 - shift_x + span_x, 1 - shift_y:1 - shift_y + span_y, 1 - shift_z:1 - shift_z + depth_z])
    return jnp.stack(pieces)

def moments(read, solid):
    density = lax.optimization_barrier(jnp.sum(read, axis=0))
    components = []
    for component in range(3):
        moment = jnp.zeros(density.shape, jnp.float32)
        for number in range(19):
            factor = int(lattice[number][component])
            if factor != 0:
                moment = moment + float(factor) * read[number]
        components.append(moment)
    momentum = jnp.stack(components)
    safe_density = jnp.where(solid, 1.0, density)
    velocity = jnp.where(solid[None], 0.0, momentum / safe_density[None])
    return (density, velocity)

def strain_size(vel_wide):
    padded = jnp.pad(vel_wide, ((0, 0), (0, 0), (0, 0), (1, 1)))
    gradient = [(padded[:, 2:, 1:-1, 1:-1] - padded[:, :-2, 1:-1, 1:-1]) * 0.5, (padded[:, 1:-1, 2:, 1:-1] - padded[:, 1:-1, :-2, 1:-1]) * 0.5, (padded[:, 1:-1, 1:-1, 2:] - padded[:, 1:-1, 1:-1, :-2]) * 0.5]
    strain_sum = jnp.zeros(gradient[0].shape[1:], jnp.float32)
    for row_axis in range(3):
        for col_axis in range(3):
            strain_ab = 0.5 * (gradient[col_axis][row_axis] + gradient[row_axis][col_axis])
            strain_sum = strain_sum + strain_ab * strain_ab
    return jnp.sqrt(2.0 * strain_sum + strain_floor)

def collide(read, density, velocity, solid, magnitude, lift_force):
    relax_time = base_tau + 3.0 * smag_coef * magnitude
    speed_sq = velocity[0] * velocity[0] + velocity[1] * velocity[1] + velocity[2] * velocity[2]
    collided = []
    for number in range(19):
        project = float(lattice[number][0]) * velocity[0] + float(lattice[number][1]) * velocity[1] + float(lattice[number][2]) * velocity[2]
        equilibrium = lattice_weight[number] * density * (1.0 + 3.0 * project + 4.5 * project * project - 1.5 * speed_sq)
        fluid_post = read[number] - (read[number] - equilibrium) / relax_time + 3.0 * lattice_weight[number] * float(lattice[number][2]) * lift_force
        collided.append(jnp.where(solid, read[opposite[number]], fluid_post))
    return jnp.stack(collided)

def lookup(heat_level, heat_table):
    heat_force = jnp.zeros(heat_level.shape, jnp.float32)
    for level_no in range(heat_table.shape[0]):
        heat_force = heat_force + jnp.where(heat_level == level_no, heat_table[level_no], 0.0)
    return heat_force

def reference(populations, heat_level, obstacle, heat_table):
    grid_y = lax.broadcasted_iota(jnp.int32, (NX, NY, NZ), 1)
    grid_z = lax.broadcasted_iota(jnp.int32, (NX, NY, NZ), 2)
    solid = (obstacle == 1) | (grid_y == 0) | (grid_y == NY - 1) | (grid_z == 0) | (grid_z == NZ - 1)
    heat_force = lookup(heat_level, heat_table)
    current = populations
    velocity = jnp.zeros((3, NX, NY, NZ), jnp.float32)
    for repeat in range(STEPS):
        padded = jnp.pad(current, ((0, 0), (1, 1), (0, 0), (0, 0)), mode='wrap')
        padded = jnp.pad(padded, ((0, 0), (0, 0), (1, 1), (1, 1)))
        read = stream_all(padded, NX, NY, NZ)
        density, velocity = moments(read, solid)
        peak_speed = jnp.max(velocity[0] * velocity[0] + velocity[1] * velocity[1] + velocity[2] * velocity[2])
        force_scale = speed_cap / jnp.sqrt(speed_cap * speed_cap + peak_speed)
        vel_wide = jnp.pad(velocity, ((0, 0), (1, 1), (0, 0), (0, 0)), mode='wrap')
        vel_wide = jnp.pad(vel_wide, ((0, 0), (0, 0), (1, 1), (0, 0)))
        magnitude = strain_size(vel_wide)
        current = collide(read, density, velocity, solid, magnitude, force_scale * heat_force)
    return (current, velocity)
```

```python
import jax
import jax.numpy as jnp
import numpy as np
from jax import lax
from jax.sharding import PartitionSpec as P

STEPS = 2


lattice = np.array(
    [
        [0, 0, 0],
        [1, 0, 0],
        [-1, 0, 0],
        [0, 1, 0],
        [0, -1, 0],
        [0, 0, 1],
        [0, 0, -1],
        [1, 1, 0],
        [-1, -1, 0],
        [1, -1, 0],
        [-1, 1, 0],
        [1, 0, 1],
        [-1, 0, -1],
        [1, 0, -1],
        [-1, 0, 1],
        [0, 1, 1],
        [0, -1, -1],
        [0, 1, -1],
        [0, -1, 1],
    ]
)
lattice_weight = [1.0 / 3.0] + [1.0 / 18.0] * 6 + [1.0 / 36.0] * 12
opposite = [0, 2, 1, 4, 3, 6, 5, 8, 7, 10, 9, 12, 11, 14, 13, 16, 15, 18, 17]
base_tau = 0.52
smag_coef = 0.04
speed_cap = 0.1
strain_floor = 1e-06


def extended_2(cells, sides, width, closed):
    for axis, dim in sides:
        count = lax.axis_size(axis)
        ends = count if closed else count - 1
        head = lax.slice_in_dim(cells, 0, width, axis=dim)
        tail = lax.slice_in_dim(cells, cells.shape[dim] - width, cells.shape[dim], axis=dim)
        cells = jnp.concatenate(
            [
                lax.ppermute(tail, axis, [(i, (i + 1) % count) for i in range(ends)]),
                cells,
                lax.ppermute(head, axis, [((i + 1) % count, i) for i in range(ends)]),
            ],
            axis=dim,
        )
    return cells


def stream_all(padded, span_x, span_y, depth_z):
    pieces = []
    for number in range(19):
        shift_x = int(lattice[number][0])
        shift_y = int(lattice[number][1])
        shift_z = int(lattice[number][2])
        pieces.append(
            padded[
                number,
                1 - shift_x : 1 - shift_x + span_x,
                1 - shift_y : 1 - shift_y + span_y,
                1 - shift_z : 1 - shift_z + depth_z,
            ]
        )
    return jnp.stack(pieces)


def moments(read, solid):
    density = jnp.sum(read, axis=0)
    components = []
    for component in range(3):
        moment = jnp.zeros(density.shape, jnp.float32)
        for number in range(19):
            factor = int(lattice[number][component])
            if factor != 0:
                moment = moment + float(factor) * read[number]
        components.append(moment)
    momentum = jnp.stack(components)
    safe_density = jnp.where(solid, 1.0, density)
    velocity = jnp.where(solid[None], 0.0, momentum / safe_density[None])
    return (density, velocity)


def strain_size(vel_wide):
    padded = jnp.pad(vel_wide, ((0, 0), (0, 0), (0, 0), (1, 1)))
    gradient = [
        (padded[:, 2:, 1:-1, 1:-1] - padded[:, :-2, 1:-1, 1:-1]) * 0.5,
        (padded[:, 1:-1, 2:, 1:-1] - padded[:, 1:-1, :-2, 1:-1]) * 0.5,
        (padded[:, 1:-1, 1:-1, 2:] - padded[:, 1:-1, 1:-1, :-2]) * 0.5,
    ]
    strain_sum = jnp.zeros(gradient[0].shape[1:], jnp.float32)
    for row_axis in range(3):
        for col_axis in range(3):
            strain_ab = 0.5 * (gradient[col_axis][row_axis] + gradient[row_axis][col_axis])
            strain_sum = strain_sum + strain_ab * strain_ab
    return jnp.sqrt(2.0 * strain_sum + strain_floor)


def collide(read, density, velocity, solid, magnitude, lift_force):
    relax_time = base_tau + 3.0 * smag_coef * magnitude
    speed_sq = velocity[0] * velocity[0] + velocity[1] * velocity[1] + velocity[2] * velocity[2]
    collided = []
    for number in range(19):
        project = (
            float(lattice[number][0]) * velocity[0]
            + float(lattice[number][1]) * velocity[1]
            + float(lattice[number][2]) * velocity[2]
        )
        equilibrium = (
            lattice_weight[number]
            * density
            * (1.0 + 3.0 * project + 4.5 * project * project - 1.5 * speed_sq)
        )
        fluid_post = (
            read[number]
            - (read[number] - equilibrium) / relax_time
            + 3.0 * lattice_weight[number] * float(lattice[number][2]) * lift_force
        )
        collided.append(jnp.where(solid, read[opposite[number]], fluid_post))
    return jnp.stack(collided)


def lookup(heat_level, heat_table):
    heat_force = jnp.zeros(heat_level.shape, jnp.float32)
    for level_no in range(heat_table.shape[0]):
        heat_force = heat_force + jnp.where(heat_level == level_no, heat_table[level_no], 0.0)
    return heat_force


def wall_flags(anchor_y, total_y, span_x, span_y, depth_z):
    grid_y = anchor_y + lax.broadcasted_iota(jnp.int32, (span_x, span_y, depth_z), 1)
    grid_z = lax.broadcasted_iota(jnp.int32, (span_x, span_y, depth_z), 2)
    return (grid_y <= 0) | (grid_y >= total_y - 1) | (grid_z == 0) | (grid_z == depth_z - 1)


def axis_max(value, axis):
    count = lax.axis_size(axis)
    if count <= 4:
        others = [
            lax.ppermute(value, axis, [(i, (i + hop) % count) for i in range(count)])
            for hop in range(1, count)
        ]
        for other in others:
            value = jnp.maximum(value, other)
        return value
    window = 1
    while window < count:
        hop = min(window, count - window)
        value = jnp.maximum(
            value, lax.ppermute(value, axis, [(i, (i + hop) % count) for i in range(count)])
        )
        window += hop
    return value


def hall_max(value):
    return axis_max(axis_max(value, "gx"), "gy")


def extend_all(stacked, rim_depth):
    extended = extended_2(stacked, (("gx", 1),), rim_depth, True)
    return extended_2(extended, (("gy", 2),), rim_depth, False)


def local(populations, heat_level, obstacle, heat_table):
    span_x = populations.shape[1]
    span_y = populations.shape[2]
    depth_z = populations.shape[3]
    anchor_y = lax.axis_index("gy") * span_y
    total_y = lax.axis_size("gy") * span_y
    solid_core = (obstacle == 1) | wall_flags(anchor_y, total_y, span_x, span_y, depth_z)
    heat_force = lookup(heat_level, heat_table)
    current = populations
    velocity = jnp.zeros((3, span_x, span_y, depth_z), jnp.float32)
    for repeat in range(STEPS):
        stacked = jnp.concatenate([current, obstacle.astype(jnp.float32)[None]], axis=0)
        extended = extend_all(stacked, 2)
        wide_pops = extended[:19]
        wide_solid = extended[19]
        padded = jnp.pad(wide_pops, ((0, 0), (0, 0), (0, 0), (1, 1)))
        read_wide = stream_all(padded, span_x + 2, span_y + 2, depth_z)
        solid_wide = (wide_solid[1:-1, 1:-1] > 0.5) | wall_flags(
            anchor_y - 1, total_y, span_x + 2, span_y + 2, depth_z
        )
        density_wide, vel_wide = moments(read_wide, solid_wide)
        read = read_wide[:, 1:-1, 1:-1]
        density = density_wide[1:-1, 1:-1]
        velocity = vel_wide[:, 1:-1, 1:-1]
        local_peak = jnp.max(
            velocity[0] * velocity[0] + velocity[1] * velocity[1] + velocity[2] * velocity[2]
        )
        peak_speed = hall_max(jnp.broadcast_to(local_peak, (8, 128)))[0, 0]
        force_scale = speed_cap / jnp.sqrt(speed_cap * speed_cap + peak_speed)
        magnitude = strain_size(vel_wide)
        current = collide(read, density, velocity, solid_core, magnitude, force_scale * heat_force)
    return (current, velocity)


def solution(mesh):
    return jax.shard_map(
        local,
        mesh=mesh,
        in_specs=(
            P(None, ("member", "gx"), "gy", None),
            P(("member", "gx"), "gy", None),
            P(("member", "gx"), "gy", None),
            P(),
        ),
        out_specs=(P(None, ("member", "gx"), "gy", None), P(None, ("member", "gx"), "gy", None)),
        check_vma=False,
    )
```

```python
import jax
import jax.numpy as jnp
import numpy as np
from jax import lax
from jax.experimental import pallas as pl
from jax.experimental.pallas import tpu as pltpu
from jax.sharding import PartitionSpec as P

STEPS = 2


lattice = np.array(
    [
        [0, 0, 0],
        [1, 0, 0],
        [-1, 0, 0],
        [0, 1, 0],
        [0, -1, 0],
        [0, 0, 1],
        [0, 0, -1],
        [1, 1, 0],
        [-1, -1, 0],
        [1, -1, 0],
        [-1, 1, 0],
        [1, 0, 1],
        [-1, 0, -1],
        [1, 0, -1],
        [-1, 0, 1],
        [0, 1, 1],
        [0, -1, -1],
        [0, 1, -1],
        [0, -1, 1],
    ]
)
lattice_weight = [1.0 / 3.0] + [1.0 / 18.0] * 6 + [1.0 / 36.0] * 12
opposite = [0, 2, 1, 4, 3, 6, 5, 8, 7, 10, 9, 12, 11, 14, 13, 16, 15, 18, 17]
base_tau = 0.52
smag_coef = 0.04
speed_cap = 0.1
strain_floor = 1e-06


LEAD = 8
shifts = [tuple(int(part) for part in row) for row in lattice]


def toward(dim, sign):
    moving = [k for k in range(19) if shifts[k][dim] == sign]
    resting = [k for k in range(19) if shifts[k][dim] == 0]
    return moving, resting


def plane_list(dim, sign):
    moving, resting = toward(dim, sign)
    return [(k, 1) for k in moving + resting] + [(k, 2) for k in moving]


N_PLANES = len(plane_list(0, 1))


def lift_coef(number):
    return 3.0 * lattice_weight[number] * float(shifts[number][2])


def first_lane(shape):
    return lax.broadcasted_iota(jnp.int32, shape, len(shape) - 1) == 0


def shift_depth(value, step):
    if step == 0:
        return value
    depth = value.shape[-1]
    lane = lax.broadcasted_iota(jnp.int32, value.shape, value.ndim - 1)
    if step > 0:
        return jnp.where(lane == 0, 0.0, pltpu.roll(value, 1, value.ndim - 1))
    return jnp.where(lane == depth - 1, 0.0, pltpu.roll(value, depth - 1, value.ndim - 1))


def pack_x_first(pops, obstacle, to_low, to_high):
    span_x = pops.shape[1]
    for out, sign in ((to_low, -1), (to_high, 1)):
        for slot, (k, far) in enumerate(plane_list(0, sign)):
            out[slot] = pops[k, far - 1 if sign < 0 else span_x - far]
        out[N_PLANES] = obstacle[0 if sign < 0 else span_x - 1].astype(jnp.float32)


def pack_y_rows(pops, from_low, from_high, own_aux, aux_far, to_low, to_high):
    span_x, span_y = pops.shape[1], pops.shape[2]
    low_slot = {item: slot for slot, item in enumerate(plane_list(0, 1))}
    high_slot = {item: slot for slot, item in enumerate(plane_list(0, -1))}
    for out, sign in ((to_low, -1), (to_high, 1)):
        for slot, (k, far) in enumerate(plane_list(1, sign)):
            row = far - 1 if sign < 0 else span_y - far
            rows = pl.ds(row, 1)
            for layer in range(span_x):
                out[slot, pl.ds(layer + 2, 1)] = pops[k, layer, rows]
            for dist in (1, 2):
                if (k, dist) in low_slot:
                    out[slot, pl.ds(2 - dist, 1)] = from_low[low_slot[(k, dist)], rows]
                if (k, dist) in high_slot:
                    out[slot, pl.ds(span_x + 1 + dist, 1)] = from_high[high_slot[(k, dist)], rows]
        for far in range(1, aux_far + 1):
            rows = pl.ds(far - 1 if sign < 0 else span_y - far, 1)
            slot = N_PLANES + far - 1
            for layer in range(span_x):
                out[slot, pl.ds(layer + 2, 1)] = own_aux[layer, rows].astype(jnp.float32)
            for dist in range(1, aux_far + 1):
                out[slot, pl.ds(2 - dist, 1)] = from_low[N_PLANES + dist - 1, rows]
                out[slot, pl.ds(span_x + 1 + dist, 1)] = from_high[N_PLANES + dist - 1, rows]


def pack_y_first(pops, obstacle, from_low, from_high, to_low, to_high):
    pack_y_rows(pops, from_low, from_high, obstacle, 1, to_low, to_high)


def stashed(plane):
    return jnp.max(jnp.where(first_lane(plane.shape), plane, 0.0))


def pack_y_second(pops, lift, peak, others, from_low, from_high, to_low, to_high, row_peak):
    pack_y_rows(pops, from_low, from_high, lift, 2, to_low, to_high)
    largest = jnp.maximum(jnp.max(peak[...]), jnp.max(others[...]))
    largest = jnp.maximum(largest, stashed(from_low[N_PLANES]))
    largest = jnp.maximum(largest, stashed(from_high[N_PLANES]))
    row_peak[...] = jnp.full(row_peak.shape, largest, jnp.float32)
    for out in (to_low, to_high):
        plane = out[N_PLANES]
        out[N_PLANES] = jnp.where(first_lane(plane.shape), largest, plane)


def widen(place, wide, pops, x_low, x_high, y_low, y_high, lift):
    span_x, span_y = pops.shape[1], pops.shape[2]
    at_low, at_high = place[0] == 0, place[0] == place[1] - 1
    own = pl.ds(LEAD, span_y)

    def with_lift(k, value, extra):
        if extra is None or shifts[k][2] == 0:
            return value
        return value + lift_coef(k) * extra

    for layer in range(span_x):
        extra = lift("own", layer)
        for k in range(19):
            wide[k, layer + 2, own] = with_lift(k, pops[k, layer], extra)
    for name, ref, sign in (("x_low", x_low, 1), ("x_high", x_high, -1)):
        extras = {far: lift(name, far) for far in (1, 2)}
        for slot, (k, far) in enumerate(plane_list(0, sign)):
            layer = 2 - far if sign > 0 else span_x + 1 + far
            wide[k, layer, own] = with_lift(k, ref[slot], extras[far])
    for name, ref, sign, wall in (("y_low", y_low, 1, at_low), ("y_high", y_high, -1, at_high)):
        extras = {far: lift(name, far) for far in (1, 2)}
        for slot, (k, far) in enumerate(plane_list(1, sign)):
            row = LEAD - far if sign > 0 else LEAD + span_y - 1 + far
            value = jnp.where(wall, 0.0, with_lift(k, ref[slot], extras[far]))
            for layer in range(span_x + 4):
                wide[k, layer, pl.ds(row, 1)] = value[layer : layer + 1]


def flow(place, wide, flags, speed):
    span_x, depth = wide.shape[1] - 4, wide.shape[3]
    span_y = wide.shape[2] - 2 * LEAD
    count = span_y + 8
    total_y = place[1] * span_y
    shape = (count, depth)
    grid_y = place[0] * span_y - 1 + lax.broadcasted_iota(jnp.int32, shape, 0)
    grid_z = lax.broadcasted_iota(jnp.int32, shape, 1)
    wall = (grid_y <= 0) | (grid_y >= total_y - 1) | (grid_z == 0) | (grid_z == depth - 1)
    for layer in range(-1, span_x + 1):
        density = None
        momentum = [None, None, None]
        for k in range(19):
            c_x, c_y, c_z = shifts[k]
            read = shift_depth(wide[k, layer + 2 - c_x, pl.ds(LEAD - 1 - c_y, count)], c_z)
            density = read if density is None else density + read
            for part in range(3):
                if shifts[k][part] != 0:
                    if momentum[part] is None:
                        momentum[part] = read * float(shifts[k][part])
                    elif shifts[k][part] > 0:
                        momentum[part] = momentum[part] + read
                    else:
                        momentum[part] = momentum[part] - read
        solid = wall | (flags[layer + 1, pl.ds(LEAD - 1, count)] > 0.5)
        inverse = 1.0 / jnp.where(solid, 1.0, density)
        for part in range(3):
            speed[part, layer + 1, pl.ds(LEAD - 1, count)] = jnp.where(
                solid, 0.0, momentum[part] * inverse
            )


def largest_speed(speed, span_x, span_y):
    most = None
    for layer in range(span_x):
        u = [speed[part, layer + 1, pl.ds(LEAD, span_y)] for part in range(3)]
        size = u[0] * u[0] + u[1] * u[1] + u[2] * u[2]
        most = size if most is None else jnp.maximum(most, size)
    return jnp.max(most)


def relax_layer(place, wide, flags, speed, layer):
    depth = wide.shape[3]
    span_y = wide.shape[2] - 2 * LEAD
    shape = (span_y, depth)
    own = pl.ds(LEAD, span_y)
    u = [speed[part, layer + 1, own] for part in range(3)]
    diff = []
    for part in range(3):
        diff.append(
            (
                speed[part, layer + 2, own] - speed[part, layer, own],
                speed[part, layer + 1, pl.ds(LEAD + 1, span_y)]
                - speed[part, layer + 1, pl.ds(LEAD - 1, span_y)],
                shift_depth(u[part], -1) - shift_depth(u[part], 1),
            )
        )
    same = diff[0][0] * diff[0][0] + diff[1][1] * diff[1][1] + diff[2][2] * diff[2][2]
    mixed = None
    for a, b in ((0, 1), (0, 2), (1, 2)):
        cross = diff[a][b] + diff[b][a]
        mixed = cross * cross if mixed is None else mixed + cross * cross
    magnitude = jnp.sqrt(0.5 * same + 0.25 * mixed + strain_floor)
    rate = 1.0 / (base_tau + 3.0 * smag_coef * magnitude)
    solid = solid_layer(place, flags, layer, shape)
    read = []
    density = None
    for k in range(19):
        c_x, c_y, c_z = shifts[k]
        value = shift_depth(wide[k, layer + 2 - c_x, pl.ds(LEAD - c_y, span_y)], c_z)
        read.append(value)
        density = value if density is None else density + value
    level = density * (1.0 - 1.5 * (u[0] * u[0] + u[1] * u[1] + u[2] * u[2]))
    fresh = [None] * 19
    keep = 1.0 - rate
    fresh[0] = jnp.where(solid, read[0], read[0] * keep + (lattice_weight[0] * rate) * level)
    for k in range(1, 19, 2):
        project = None
        for part in range(3):
            if shifts[k][part] != 0:
                term = u[part] if shifts[k][part] > 0 else -u[part]
                project = term if project is None else project + term
        even = level + density * (4.5 * project * project)
        odd = density * (3.0 * project)
        scaled = lattice_weight[k] * rate
        fresh[k] = jnp.where(solid, read[k + 1], read[k] * keep + scaled * (even + odd))
        fresh[k + 1] = jnp.where(solid, read[k], read[k + 1] * keep + scaled * (even - odd))
    return fresh, solid


def solid_layer(place, flags, layer, shape):
    span_y, depth = shape
    grid_y = place[0] * span_y + lax.broadcasted_iota(jnp.int32, shape, 0)
    grid_z = lax.broadcasted_iota(jnp.int32, shape, 1)
    wall = (grid_y <= 0) | (grid_y >= place[1] * span_y - 1) | (grid_z == 0) | (grid_z == depth - 1)
    return wall | (flags[layer + 1, pl.ds(LEAD, span_y)] > 0.5)


def step_first(
    place, table, pops, obstacle, heat_level, x_low, x_high, y_low, y_high,
    fresh_out, flags, lift_out, peak, to_low, to_high, wide, speed,
):
    span_x, span_y, depth = pops.shape[1:]
    own = pl.ds(LEAD, span_y)
    for layer in range(span_x):
        flags[layer + 1, own] = obstacle[layer].astype(jnp.float32)
        flags[layer + 1, pl.ds(LEAD - 1, 1)] = y_low[N_PLANES, pl.ds(layer + 2, 1)]
        flags[layer + 1, pl.ds(LEAD + span_y, 1)] = y_high[N_PLANES, pl.ds(layer + 2, 1)]
    flags[0, own] = x_low[N_PLANES]
    flags[span_x + 1, own] = x_high[N_PLANES]
    widen(place, wide, pops, x_low, x_high, y_low, y_high, lambda name, far: None)
    flow(place, wide, flags, speed)
    most = largest_speed(speed, span_x, span_y)
    peak[...] = jnp.full(peak.shape, most, jnp.float32)
    outs = ((to_low, -1), (to_high, 1))
    slots = {sign: {item: n for n, item in enumerate(plane_list(0, sign))} for sign in (-1, 1)}
    for layer in range(span_x):
        fresh, solid = relax_layer(place, wide, flags, speed, layer)
        force = jnp.zeros((span_y, depth), jnp.float32)
        for level_no in range(table.shape[0]):
            force = jnp.where(heat_level[layer] == level_no, table[level_no], force)
        force = jnp.where(solid, 0.0, force)
        lift_out[layer] = force
        for k in range(19):
            fresh_out[k, layer] = fresh[k]
        for out, sign in outs:
            far = layer + 1 if sign < 0 else span_x - layer
            if far <= 2:
                for k in range(19):
                    if (k, far) in slots[sign]:
                        out[slots[sign][(k, far)]] = fresh[k]
                extra = jnp.where(first_lane(force.shape), most, force) if far == 1 else force
                out[N_PLANES + far - 1] = extra


def step_second(
    place, pops, lift, flags, x_low, x_high, y_low, y_high, row_peak, others,
    fresh_out, speed_out, peak, wide, speed,
):
    span_x, span_y, depth = pops.shape[1:]
    largest = jnp.maximum(jnp.max(row_peak[...]), jnp.max(others[...]))
    largest = jnp.maximum(largest, stashed(y_low[N_PLANES]))
    largest = jnp.maximum(largest, stashed(y_high[N_PLANES]))
    scale = speed_cap / jnp.sqrt(speed_cap * speed_cap + jnp.full((1, depth), largest, jnp.float32))

    refs = {"x_low": x_low, "x_high": x_high, "y_low": y_low, "y_high": y_high}

    def scaled(name, far):
        if name == "own":
            return scale * lift[far]
        plane = refs[name][N_PLANES + far - 1]
        return scale * jnp.where(first_lane(plane.shape), 0.0, plane)

    widen(place, wide, pops, x_low, x_high, y_low, y_high, scaled)
    flow(place, wide, flags, speed)
    peak[...] = jnp.full(peak.shape, largest_speed(speed, span_x, span_y), jnp.float32)
    for layer in range(span_x):
        for part in range(3):
            speed_out[part, layer] = speed[part, layer + 1, pl.ds(LEAD, span_y)]
        fresh, _ = relax_layer(place, wide, flags, speed, layer)
        for k in range(19):
            fresh_out[k, layer] = fresh[k]


def ring(value, axis, hop, closed=True):
    count = lax.axis_size(axis)
    pairs = [(i, i + hop) for i in range(count)]
    if closed:
        pairs = [(i, j % count) for i, j in pairs]
    else:
        pairs = [(i, j) for i, j in pairs if 0 <= j < count]
    return lax.ppermute(value, axis, pairs)


def axis_max(value, axis):
    count = lax.axis_size(axis)
    if count <= 4:
        for other in [ring(value, axis, hop) for hop in range(1, count)]:
            value = jnp.maximum(value, other)
        return value
    window = 1
    while window < count:
        hop = min(window, count - window)
        value = jnp.maximum(value, ring(value, axis, hop))
        window += hop
    return value


def beyond(value, axis):
    count = lax.axis_size(axis)
    if count <= 3:
        return value
    if count == 4:
        return ring(value, axis, 2)
    return axis_max(value, axis)


def shaped(*dims):
    return jax.ShapeDtypeStruct(dims, jnp.float32)


def call(kernel, outs, spaces, scratch=()):
    return pl.pallas_call(
        kernel,
        out_shape=outs,
        in_specs=[pl.BlockSpec(memory_space=space) for space in spaces],
        out_specs=[pl.BlockSpec(memory_space=pltpu.VMEM) for _ in outs],
        scratch_shapes=list(scratch),
        compiler_params=pltpu.CompilerParams(vmem_limit_bytes=40 * 1024 * 1024),
    )


def local(populations, heat_level, obstacle, heat_table):
    _, span_x, span_y, depth = populations.shape
    vmem, smem = pltpu.VMEM, pltpu.SMEM
    place = jnp.stack([lax.axis_index("gy"), lax.axis_size("gy")]).astype(jnp.int32)
    block = shaped(19, span_x, span_y, depth)
    small = shaped(8, depth)
    scratch = (
        pltpu.VMEM((19, span_x + 4, span_y + 2 * LEAD, depth), jnp.float32),
        pltpu.VMEM((3, span_x + 2, span_y + 2 * LEAD, depth), jnp.float32),
    )

    x_face = shaped(N_PLANES + 1, span_y, depth)
    y_face = shaped(N_PLANES + 1, span_x + 4, depth)
    to_low, to_high = call(pack_x_first, [x_face] * 2, [vmem] * 2)(populations, obstacle)
    x_low, x_high = ring(to_high, "gx", 1), ring(to_low, "gx", -1)
    to_low, to_high = call(pack_y_first, [y_face] * 2, [vmem] * 4)(
        populations, obstacle, x_low, x_high
    )
    y_low, y_high = ring(to_high, "gy", 1, False), ring(to_low, "gy", -1, False)

    x_face = shaped(N_PLANES + 2, span_y, depth)
    y_face = shaped(N_PLANES + 2, span_x + 4, depth)
    flags = shaped(span_x + 2, span_y + 2 * LEAD, depth)
    current, flags, lift, peak, to_low, to_high = call(
        step_first,
        [block, flags, shaped(span_x, span_y, depth), small, x_face, x_face],
        [smem, smem] + [vmem] * 7,
        scratch,
    )(place, heat_table, populations, obstacle, heat_level, x_low, x_high, y_low, y_high)
    x_low, x_high = ring(to_high, "gx", 1), ring(to_low, "gx", -1)
    others = beyond(peak, "gx")
    to_low, to_high, row_peak = call(pack_y_second, [y_face, y_face, small], [vmem] * 6)(
        current, lift, peak, others, x_low, x_high
    )
    y_low, y_high = ring(to_high, "gy", 1), ring(to_low, "gy", -1)
    others = beyond(row_peak, "gy")
    current, velocity, peak = call(
        step_second,
        [block, shaped(3, span_x, span_y, depth), small],
        [smem] + [vmem] * 9,
        scratch,
    )(place, current, lift, flags, x_low, x_high, y_low, y_high, row_peak, others)

    peak = axis_max(axis_max(peak, "gx"), "gy")[0, 0]
    force_scale = speed_cap / jnp.sqrt(speed_cap * speed_cap + peak)
    coef = jnp.array([lift_coef(k) for k in range(19)], jnp.float32)
    current = current + coef[:, None, None, None] * (force_scale * lift)[None]
    return (current, velocity)


def solution(mesh):
    return jax.shard_map(
        local,
        mesh=mesh,
        in_specs=(
            P(None, ("member", "gx"), "gy", None),
            P(("member", "gx"), "gy", None),
            P(("member", "gx"), "gy", None),
            P(),
        ),
        out_specs=(P(None, ("member", "gx"), "gy", None), P(None, ("member", "gx"), "gy", None)),
        check_vma=False,
    )
```

```python
import jax
import jax.numpy as jnp
import numpy as np
from jax import lax
from jax.experimental import pallas as pl
from jax.experimental.pallas import tpu as pltpu
from jax.sharding import PartitionSpec as P

STEPS = 2


lattice = np.array(
    [
        [0, 0, 0],
        [1, 0, 0],
        [-1, 0, 0],
        [0, 1, 0],
        [0, -1, 0],
        [0, 0, 1],
        [0, 0, -1],
        [1, 1, 0],
        [-1, -1, 0],
        [1, -1, 0],
        [-1, 1, 0],
        [1, 0, 1],
        [-1, 0, -1],
        [1, 0, -1],
        [-1, 0, 1],
        [0, 1, 1],
        [0, -1, -1],
        [0, 1, -1],
        [0, -1, 1],
    ]
)
lattice_weight = [1.0 / 3.0] + [1.0 / 18.0] * 6 + [1.0 / 36.0] * 12
opposite = [0, 2, 1, 4, 3, 6, 5, 8, 7, 10, 9, 12, 11, 14, 13, 16, 15, 18, 17]
base_tau = 0.52
smag_coef = 0.04
speed_cap = 0.1
strain_floor = 1e-06


LEAD = 8
shifts = [tuple(int(part) for part in row) for row in lattice]


def moving(dim, sign):
    return [k for k in range(19) if shifts[k][dim] == sign]


def reached(dim, sign):
    resting = [k for k in range(19) if shifts[k][dim] == 0]
    return [(k, 1) for k in moving(dim, sign) + resting] + [(k, 2) for k in moving(dim, sign)]


def corner_rows(sign):
    rows = []
    for sign_y in (1, -1):
        for k in range(19):
            if shifts[k][1] == sign_y and shifts[k][0] == 0:
                rows.append((k, 1, sign_y))
            if shifts[k][1] == sign_y and shifts[k][0] == sign:
                rows.append((k, 2, sign_y))
    return rows


N_MOVING = len(moving(0, 1))
N_SUMS = 4
CORNERS = N_MOVING + N_SUMS
AUX_X = CORNERS + 1
AUX_Y = N_MOVING + N_SUMS


def lift_coef(number):
    return 3.0 * lattice_weight[number] * float(shifts[number][2])


def first_lane(shape):
    return lax.broadcasted_iota(jnp.int32, shape, len(shape) - 1) == 0


def shift_depth(value, step):
    if step == 0:
        return value
    depth = value.shape[-1]
    lane = lax.broadcasted_iota(jnp.int32, value.shape, value.ndim - 1)
    if step > 0:
        return jnp.where(lane == 0, 0.0, pltpu.roll(value, 1, value.ndim - 1))
    return jnp.where(lane == depth - 1, 0.0, pltpu.roll(value, depth - 1, value.ndim - 1))


def gather_sums(terms):
    sums = [None] * N_SUMS
    for k, read in terms:
        for part, factor in enumerate((1,) + shifts[k]):
            if factor != 0:
                value = read if factor > 0 else -read
                sums[part] = value if sums[part] is None else sums[part] + value
    return sums


def shift_rows(value, step):
    if step == 0:
        return value
    count = value.shape[0]
    row = lax.broadcasted_iota(jnp.int32, value.shape, 0)
    if step > 0:
        return jnp.where(row == 0, 0.0, pltpu.roll(value, 1, 0))
    return jnp.where(row == count - 1, 0.0, pltpu.roll(value, count - 1, 0))


def pack_x(state, to_low, to_high):
    span_x, span_y = state.shape[1], state.shape[2]
    for out, sign in ((to_low, -1), (to_high, 1)):
        layers = {far: far - 1 if sign < 0 else span_x - far for far in (1, 2)}
        for slot, k in enumerate(moving(0, sign)):
            out[slot] = state[k, layers[1]]
        terms = []
        for k, far in reached(0, sign):
            if far == 2 or shifts[k][0] == 0:
                value = shift_rows(state[k, layers[far]], shifts[k][1])
                terms.append((k, shift_depth(value, shifts[k][2])))
        for part, value in enumerate(gather_sums(terms)):
            out[N_MOVING + part] = value
        for slot, (k, far, sign_y) in enumerate(corner_rows(sign)):
            row = 0 if sign_y < 0 else span_y - 1
            out[CORNERS, pl.ds(slot, 1)] = state[k, layers[far], pl.ds(row, 1)]


def pack_x_first(pops, obstacle, to_low, to_high):
    pack_x(pops, to_low, to_high)
    to_low[AUX_X] = obstacle[0].astype(jnp.float32)
    to_high[AUX_X] = obstacle[obstacle.shape[0] - 1].astype(jnp.float32)


def pack_y_rows(pops, from_low, from_high, own_aux, aux_far, to_low, to_high, rows_of):
    span_x, span_y = pops.shape[1], pops.shape[2]
    sides = ((from_low, 1), (from_high, -1))
    for out, sign in ((to_low, -1), (to_high, 1)):
        slots = {k: slot for slot, k in enumerate(moving(1, sign))}
        terms = []
        for number, (k, far) in enumerate(reached(1, sign)):
            sent = far == 1 and k in slots
            rows = pl.ds(far - 1 if sign < 0 else span_y - far, 1)
            plane = out.at[slots[k]] if sent else rows_of.at[number]
            for layer in range(span_x):
                plane[pl.ds(layer + 2, 1)] = pops[k, layer, rows]
            for source, sign_x in sides:
                near = 1 if sign_x > 0 else span_x + 2
                if k in moving(0, sign_x):
                    plane[pl.ds(near, 1)] = source[moving(0, sign_x).index(k), rows]
                if sent:
                    for slot, (other, dist, sign_y) in enumerate(corner_rows(sign_x)):
                        if other == k and sign_y == sign:
                            x = near if dist == 1 else near - sign_x
                            plane[pl.ds(x, 1)] = source[CORNERS, pl.ds(slot, 1)]
            if not sent:
                terms.append((k, plane))
        reads = []
        for k, plane in terms:
            value = plane[...]
            if shifts[k][0] != 0:
                value = pltpu.roll(value, shifts[k][0] % value.shape[0], 0)
            reads.append((k, shift_depth(value, shifts[k][2])))
        for part, value in enumerate(gather_sums(reads)):
            out[N_MOVING + part] = value
        for far in range(1, aux_far + 1):
            rows = pl.ds(far - 1 if sign < 0 else span_y - far, 1)
            slot = AUX_Y + far - 1
            for layer in range(span_x):
                out[slot, pl.ds(layer + 2, 1)] = own_aux[layer, rows].astype(jnp.float32)
            for dist in range(1, aux_far + 1):
                out[slot, pl.ds(2 - dist, 1)] = from_low[AUX_X + dist - 1, rows]
                out[slot, pl.ds(span_x + 1 + dist, 1)] = from_high[AUX_X + dist - 1, rows]


def pack_y_first(pops, obstacle, from_low, from_high, to_low, to_high, rows_of):
    pack_y_rows(pops, from_low, from_high, obstacle, 1, to_low, to_high, rows_of)


def stashed(plane):
    return jnp.max(jnp.where(first_lane(plane.shape), plane, 0.0))


def pack_y_second(pops, lift, peak, others, from_low, from_high, to_low, to_high, row_peak, rows_of):
    pack_y_rows(pops, from_low, from_high, lift, 2, to_low, to_high, rows_of)
    largest = jnp.maximum(jnp.max(peak[...]), jnp.max(others[...]))
    largest = jnp.maximum(largest, stashed(from_low[AUX_X]))
    largest = jnp.maximum(largest, stashed(from_high[AUX_X]))
    row_peak[...] = jnp.full(row_peak.shape, largest, jnp.float32)
    for out in (to_low, to_high):
        plane = out[AUX_Y]
        out[AUX_Y] = jnp.where(first_lane(plane.shape), largest, plane)


def widen(place, wide, sums, pops, x_low, x_high, y_low, y_high, lift):
    span_x, span_y = pops.shape[1], pops.shape[2]
    at_low, at_high = place[0] == 0, place[0] == place[1] - 1
    own = pl.ds(LEAD, span_y)

    def with_lift(k, value, extra):
        if extra is None or shifts[k][2] == 0:
            return value
        return value + lift_coef(k) * extra

    for layer in range(span_x):
        extra = lift("own", layer)
        for k in range(19):
            wide[k, layer + 2, own] = with_lift(k, pops[k, layer], extra)
    sums[...] = jnp.zeros(sums.shape, jnp.float32)
    blank = jnp.zeros((span_y, pops.shape[3]), jnp.float32)
    for name, ref, sign in (("x_low", x_low, 1), ("x_high", x_high, -1)):
        extras = {far: lift(name, far) for far in (1, 2)}
        for k, far in reached(0, sign):
            layer = 2 - far if sign > 0 else span_x + 1 + far
            sent = far == 1 and k in moving(0, sign)
            value = ref[moving(0, sign).index(k)] if sent else blank
            wide[k, layer, own] = with_lift(k, value, extras[far])
        for part in range(N_SUMS):
            sums[part, 0 if sign > 0 else span_x + 1, own] = ref[N_MOVING + part]
    blank = jnp.zeros((span_x + 4, pops.shape[3]), jnp.float32)
    for name, ref, sign, wall in (("y_low", y_low, 1, at_low), ("y_high", y_high, -1, at_high)):
        extras = {far: lift(name, far) for far in (1, 2)}
        for k, far in reached(1, sign):
            row = LEAD - far if sign > 0 else LEAD + span_y - 1 + far
            sent = far == 1 and k in moving(1, sign)
            value = with_lift(k, ref[moving(1, sign).index(k)] if sent else blank, extras[far])
            if sent or shifts[k][2] != 0:
                value = jnp.where(wall, 0.0, value)
            for layer in range(span_x + 4):
                wide[k, layer, pl.ds(row, 1)] = value[layer : layer + 1]
        row = LEAD - 1 if sign > 0 else LEAD + span_y
        for part in range(N_SUMS):
            for layer in range(span_x):
                sums[part, layer + 1, pl.ds(row, 1)] = ref[N_MOVING + part, pl.ds(layer + 2, 1)]


def flow(place, wide, sums, flags, speed):
    span_x, depth = wide.shape[1] - 4, wide.shape[3]
    span_y = wide.shape[2] - 2 * LEAD
    count = span_y + 8
    total_y = place[1] * span_y
    shape = (count, depth)
    grid_y = place[0] * span_y - 1 + lax.broadcasted_iota(jnp.int32, shape, 0)
    grid_z = lax.broadcasted_iota(jnp.int32, shape, 1)
    wall = (grid_y <= 0) | (grid_y >= total_y - 1) | (grid_z == 0) | (grid_z == depth - 1)
    for layer in range(-1, span_x + 1):
        rows = pl.ds(LEAD - 1, count)
        density, *momentum = [sums[part, layer + 1, rows] for part in range(N_SUMS)]
        for k in range(19):
            c_x, c_y, c_z = shifts[k]
            read = shift_depth(wide[k, layer + 2 - c_x, pl.ds(LEAD - 1 - c_y, count)], c_z)
            density = density + read
            for part in range(3):
                if shifts[k][part] > 0:
                    momentum[part] = momentum[part] + read
                elif shifts[k][part] < 0:
                    momentum[part] = momentum[part] - read
        solid = wall | (flags[layer + 1, pl.ds(LEAD - 1, count)] > 0.5)
        inverse = 1.0 / jnp.where(solid, 1.0, density)
        for part in range(3):
            speed[part, layer + 1, pl.ds(LEAD - 1, count)] = jnp.where(
                solid, 0.0, momentum[part] * inverse
            )


def largest_speed(speed, span_x, span_y):
    most = None
    for layer in range(span_x):
        u = [speed[part, layer + 1, pl.ds(LEAD, span_y)] for part in range(3)]
        size = u[0] * u[0] + u[1] * u[1] + u[2] * u[2]
        most = size if most is None else jnp.maximum(most, size)
    return jnp.max(most)


def relax_layer(place, wide, flags, speed, layer):
    depth = wide.shape[3]
    span_y = wide.shape[2] - 2 * LEAD
    shape = (span_y, depth)
    own = pl.ds(LEAD, span_y)
    u = [speed[part, layer + 1, own] for part in range(3)]
    diff = []
    for part in range(3):
        diff.append(
            (
                speed[part, layer + 2, own] - speed[part, layer, own],
                speed[part, layer + 1, pl.ds(LEAD + 1, span_y)]
                - speed[part, layer + 1, pl.ds(LEAD - 1, span_y)],
                shift_depth(u[part], -1) - shift_depth(u[part], 1),
            )
        )
    same = diff[0][0] * diff[0][0] + diff[1][1] * diff[1][1] + diff[2][2] * diff[2][2]
    mixed = None
    for a, b in ((0, 1), (0, 2), (1, 2)):
        cross = diff[a][b] + diff[b][a]
        mixed = cross * cross if mixed is None else mixed + cross * cross
    magnitude = jnp.sqrt(0.5 * same + 0.25 * mixed + strain_floor)
    rate = 1.0 / (base_tau + 3.0 * smag_coef * magnitude)
    solid = solid_layer(place, flags, layer, shape)
    read = []
    density = None
    for k in range(19):
        c_x, c_y, c_z = shifts[k]
        value = shift_depth(wide[k, layer + 2 - c_x, pl.ds(LEAD - c_y, span_y)], c_z)
        read.append(value)
        density = value if density is None else density + value
    level = density * (1.0 - 1.5 * (u[0] * u[0] + u[1] * u[1] + u[2] * u[2]))
    fresh = [None] * 19
    keep = 1.0 - rate
    fresh[0] = jnp.where(solid, read[0], read[0] * keep + (lattice_weight[0] * rate) * level)
    for k in range(1, 19, 2):
        project = None
        for part in range(3):
            if shifts[k][part] != 0:
                term = u[part] if shifts[k][part] > 0 else -u[part]
                project = term if project is None else project + term
        even = level + density * (4.5 * project * project)
        odd = density * (3.0 * project)
        scaled = lattice_weight[k] * rate
        fresh[k] = jnp.where(solid, read[k + 1], read[k] * keep + scaled * (even + odd))
        fresh[k + 1] = jnp.where(solid, read[k], read[k + 1] * keep + scaled * (even - odd))
    return fresh, solid


def solid_layer(place, flags, layer, shape):
    span_y, depth = shape
    grid_y = place[0] * span_y + lax.broadcasted_iota(jnp.int32, shape, 0)
    grid_z = lax.broadcasted_iota(jnp.int32, shape, 1)
    wall = (grid_y <= 0) | (grid_y >= place[1] * span_y - 1) | (grid_z == 0) | (grid_z == depth - 1)
    return wall | (flags[layer + 1, pl.ds(LEAD, span_y)] > 0.5)


def step_first(
    place, table, pops, obstacle, heat_level, x_low, x_high, y_low, y_high,
    fresh_out, flags, lift_out, peak, to_low, to_high, wide, speed, sums,
):
    span_x, span_y, depth = pops.shape[1:]
    own = pl.ds(LEAD, span_y)
    for layer in range(span_x):
        flags[layer + 1, own] = obstacle[layer].astype(jnp.float32)
        flags[layer + 1, pl.ds(LEAD - 1, 1)] = y_low[AUX_Y, pl.ds(layer + 2, 1)]
        flags[layer + 1, pl.ds(LEAD + span_y, 1)] = y_high[AUX_Y, pl.ds(layer + 2, 1)]
    flags[0, own] = x_low[AUX_X]
    flags[span_x + 1, own] = x_high[AUX_X]
    widen(place, wide, sums, pops, x_low, x_high, y_low, y_high, lambda name, far: None)
    flow(place, wide, sums, flags, speed)
    most = largest_speed(speed, span_x, span_y)
    peak[...] = jnp.full(peak.shape, most, jnp.float32)
    outs = ((to_low, -1), (to_high, 1))
    for layer in range(span_x):
        fresh, solid = relax_layer(place, wide, flags, speed, layer)
        force = jnp.zeros((span_y, depth), jnp.float32)
        for level_no in range(table.shape[0]):
            force = jnp.where(heat_level[layer] == level_no, table[level_no], force)
        force = jnp.where(solid, 0.0, force)
        lift_out[layer] = force
        for k in range(19):
            fresh_out[k, layer] = fresh[k]
        for out, sign in outs:
            far = layer + 1 if sign < 0 else span_x - layer
            if far <= 2:
                extra = jnp.where(first_lane(force.shape), most, force) if far == 1 else force
                out[AUX_X + far - 1] = extra
    pack_x(fresh_out, to_low, to_high)


def step_second(
    place, pops, lift, flags, x_low, x_high, y_low, y_high, row_peak, others,
    fresh_out, speed_out, peak, wide, speed, sums,
):
    span_x, span_y, depth = pops.shape[1:]
    largest = jnp.maximum(jnp.max(row_peak[...]), jnp.max(others[...]))
    largest = jnp.maximum(largest, stashed(y_low[AUX_Y]))
    largest = jnp.maximum(largest, stashed(y_high[AUX_Y]))
    scale = speed_cap / jnp.sqrt(speed_cap * speed_cap + jnp.full((1, depth), largest, jnp.float32))

    planes = {
        "x_low": (x_low, AUX_X),
        "x_high": (x_high, AUX_X),
        "y_low": (y_low, AUX_Y),
        "y_high": (y_high, AUX_Y),
    }

    def scaled(name, far):
        if name == "own":
            return scale * lift[far]
        ref, first = planes[name]
        plane = ref[first + far - 1]
        return scale * jnp.where(first_lane(plane.shape), 0.0, plane)

    widen(place, wide, sums, pops, x_low, x_high, y_low, y_high, scaled)
    flow(place, wide, sums, flags, speed)
    peak[...] = jnp.full(peak.shape, largest_speed(speed, span_x, span_y), jnp.float32)
    for layer in range(span_x):
        for part in range(3):
            speed_out[part, layer] = speed[part, layer + 1, pl.ds(LEAD, span_y)]
        fresh, _ = relax_layer(place, wide, flags, speed, layer)
        for k in range(19):
            fresh_out[k, layer] = fresh[k]


def ring(value, axis, hop, closed=True):
    count = lax.axis_size(axis)
    pairs = [(i, i + hop) for i in range(count)]
    if closed:
        pairs = [(i, j % count) for i, j in pairs]
    else:
        pairs = [(i, j) for i, j in pairs if 0 <= j < count]
    return lax.ppermute(value, axis, pairs)


def axis_max(value, axis):
    count = lax.axis_size(axis)
    if count <= 4:
        for other in [ring(value, axis, hop) for hop in range(1, count)]:
            value = jnp.maximum(value, other)
        return value
    window = 1
    while window < count:
        hop = min(window, count - window)
        value = jnp.maximum(value, ring(value, axis, hop))
        window += hop
    return value


def beyond(value, axis):
    count = lax.axis_size(axis)
    if count <= 3:
        return value
    if count == 4:
        return ring(value, axis, 2)
    return axis_max(value, axis)


def shaped(*dims):
    return jax.ShapeDtypeStruct(dims, jnp.float32)


def call(kernel, outs, spaces, scratch=()):
    return pl.pallas_call(
        kernel,
        out_shape=outs,
        in_specs=[pl.BlockSpec(memory_space=space) for space in spaces],
        out_specs=[pl.BlockSpec(memory_space=pltpu.VMEM) for _ in outs],
        scratch_shapes=list(scratch),
        compiler_params=pltpu.CompilerParams(vmem_limit_bytes=40 * 1024 * 1024),
    )


def local(populations, heat_level, obstacle, heat_table):
    _, span_x, span_y, depth = populations.shape
    vmem, smem = pltpu.VMEM, pltpu.SMEM
    place = jnp.stack([lax.axis_index("gy"), lax.axis_size("gy")]).astype(jnp.int32)
    block = shaped(19, span_x, span_y, depth)
    small = shaped(8, depth)
    scratch = (
        pltpu.VMEM((19, span_x + 4, span_y + 2 * LEAD, depth), jnp.float32),
        pltpu.VMEM((3, span_x + 2, span_y + 2 * LEAD, depth), jnp.float32),
        pltpu.VMEM((N_SUMS, span_x + 2, span_y + 2 * LEAD, depth), jnp.float32),
    )
    rows_of = [pltpu.VMEM((len(reached(1, 1)), span_x + 4, depth), jnp.float32)]

    x_face = shaped(AUX_X + 1, span_y, depth)
    y_face = shaped(AUX_Y + 1, span_x + 4, depth)
    to_low, to_high = call(pack_x_first, [x_face] * 2, [vmem] * 2)(populations, obstacle)
    x_low, x_high = ring(to_high, "gx", 1), ring(to_low, "gx", -1)
    to_low, to_high = call(pack_y_first, [y_face] * 2, [vmem] * 4, rows_of)(
        populations, obstacle, x_low, x_high
    )
    y_low, y_high = ring(to_high, "gy", 1, False), ring(to_low, "gy", -1, False)

    x_face = shaped(AUX_X + 2, span_y, depth)
    y_face = shaped(AUX_Y + 2, span_x + 4, depth)
    flags = shaped(span_x + 2, span_y + 2 * LEAD, depth)
    current, flags, lift, peak, to_low, to_high = call(
        step_first,
        [block, flags, shaped(span_x, span_y, depth), small, x_face, x_face],
        [smem, smem] + [vmem] * 7,
        scratch,
    )(place, heat_table, populations, obstacle, heat_level, x_low, x_high, y_low, y_high)
    x_low, x_high = ring(to_high, "gx", 1), ring(to_low, "gx", -1)
    others = beyond(peak, "gx")
    to_low, to_high, row_peak = call(pack_y_second, [y_face, y_face, small], [vmem] * 6, rows_of)(
        current, lift, peak, others, x_low, x_high
    )
    y_low, y_high = ring(to_high, "gy", 1), ring(to_low, "gy", -1)
    others = beyond(row_peak, "gy")
    current, velocity, peak = call(
        step_second,
        [block, shaped(3, span_x, span_y, depth), small],
        [smem] + [vmem] * 9,
        scratch,
    )(place, current, lift, flags, x_low, x_high, y_low, y_high, row_peak, others)

    peak = axis_max(axis_max(peak, "gx"), "gy")[0, 0]
    force_scale = speed_cap / jnp.sqrt(speed_cap * speed_cap + peak)
    coef = jnp.array([lift_coef(k) for k in range(19)], jnp.float32)
    current = current + coef[:, None, None, None] * (force_scale * lift)[None]
    return (current, velocity)


def solution(mesh):
    return jax.shard_map(
        local,
        mesh=mesh,
        in_specs=(
            P(None, ("member", "gx"), "gy", None),
            P(("member", "gx"), "gy", None),
            P(("member", "gx"), "gy", None),
            P(),
        ),
        out_specs=(P(None, ("member", "gx"), "gy", None), P(None, ("member", "gx"), "gy", None)),
        check_vma=False,
    )
```

```python
import jax
import jax.numpy as jnp
import numpy as np
from jax import lax
from jax.experimental import pallas as pl
from jax.experimental.pallas import tpu as pltpu
from jax.sharding import PartitionSpec as P

STEPS = 2


lattice = np.array(
    [
        [0, 0, 0],
        [1, 0, 0],
        [-1, 0, 0],
        [0, 1, 0],
        [0, -1, 0],
        [0, 0, 1],
        [0, 0, -1],
        [1, 1, 0],
        [-1, -1, 0],
        [1, -1, 0],
        [-1, 1, 0],
        [1, 0, 1],
        [-1, 0, -1],
        [1, 0, -1],
        [-1, 0, 1],
        [0, 1, 1],
        [0, -1, -1],
        [0, 1, -1],
        [0, -1, 1],
    ]
)
lattice_weight = [1.0 / 3.0] + [1.0 / 18.0] * 6 + [1.0 / 36.0] * 12
opposite = [0, 2, 1, 4, 3, 6, 5, 8, 7, 10, 9, 12, 11, 14, 13, 16, 15, 18, 17]
base_tau = 0.52
smag_coef = 0.04
speed_cap = 0.1
strain_floor = 1e-06


LEAD = 8
shifts = [tuple(int(part) for part in row) for row in lattice]


def moving(dim, sign):
    return [k for k in range(19) if shifts[k][dim] == sign]


def reached(dim, sign):
    resting = [k for k in range(19) if shifts[k][dim] == 0]
    return [(k, 1) for k in moving(dim, sign) + resting] + [(k, 2) for k in moving(dim, sign)]


def corner_rows(sign):
    rows = []
    for sign_y in (1, -1):
        for k in range(19):
            if shifts[k][1] == sign_y and shifts[k][0] == 0:
                rows.append((k, 1, sign_y))
            if shifts[k][1] == sign_y and shifts[k][0] == sign:
                rows.append((k, 2, sign_y))
    return rows


N_MOVING = len(moving(0, 1))
N_SUMS = 4
CORNERS = N_MOVING + N_SUMS
AUX_X = CORNERS + 1
AUX_Y = N_MOVING + N_SUMS


def lift_coef(number):
    return 3.0 * lattice_weight[number] * float(shifts[number][2])


def first_lane(shape):
    return lax.broadcasted_iota(jnp.int32, shape, len(shape) - 1) == 0


def shift_depth(value, step):
    if step == 0:
        return value
    depth = value.shape[-1]
    lane = lax.broadcasted_iota(jnp.int32, value.shape, value.ndim - 1)
    if step > 0:
        return jnp.where(lane == 0, 0.0, pltpu.roll(value, 1, value.ndim - 1))
    return jnp.where(lane == depth - 1, 0.0, pltpu.roll(value, depth - 1, value.ndim - 1))


def gather_sums(terms):
    sums = [None] * N_SUMS
    for k, read in terms:
        for part, factor in enumerate((1,) + shifts[k]):
            if factor != 0:
                value = read if factor > 0 else -read
                sums[part] = value if sums[part] is None else sums[part] + value
    return sums


def shift_rows(value, step):
    if step == 0:
        return value
    count = value.shape[0]
    row = lax.broadcasted_iota(jnp.int32, value.shape, 0)
    if step > 0:
        return jnp.where(row == 0, 0.0, pltpu.roll(value, 1, 0))
    return jnp.where(row == count - 1, 0.0, pltpu.roll(value, count - 1, 0))


def pack_x(state, to_low, to_high):
    span_x, span_y = state.shape[1], state.shape[2]
    for out, sign in ((to_low, -1), (to_high, 1)):
        layers = {far: far - 1 if sign < 0 else span_x - far for far in (1, 2)}
        for slot, k in enumerate(moving(0, sign)):
            out[slot] = state[k, layers[1]]
        terms = []
        for k, far in reached(0, sign):
            if far == 2 or shifts[k][0] == 0:
                value = shift_rows(state[k, layers[far]], shifts[k][1])
                terms.append((k, shift_depth(value, shifts[k][2])))
        for part, value in enumerate(gather_sums(terms)):
            out[N_MOVING + part] = value
        for slot, (k, far, sign_y) in enumerate(corner_rows(sign)):
            row = 0 if sign_y < 0 else span_y - 1
            out[CORNERS, pl.ds(slot, 1)] = state[k, layers[far], pl.ds(row, 1)]


def pack_x_first(pops, obstacle, to_low, to_high, stage, stage_solid, done, done_solid):
    span_x = pops.shape[1]
    first = []
    for sign in (-1, 1):
        for k, far in reached(0, sign):
            piece = (k, far - 1 if sign < 0 else span_x - far)
            if piece not in first:
                first.append(piece)
    rest = [(k, layer) for k in range(19) for layer in range(span_x) if (k, layer) not in first]
    copies = [
        pltpu.make_async_copy(pops.at[k, layer], stage.at[k, layer], done.at[number])
        for number, (k, layer) in enumerate(first + rest)
    ]
    flags = pltpu.make_async_copy(obstacle, stage_solid, done_solid.at[0])
    for copy in copies[: len(first)]:
        copy.start()
    flags.start()
    for copy in copies[len(first) :]:
        copy.start()
    for copy in copies[: len(first)]:
        copy.wait()
    pack_x(stage, to_low, to_high)
    flags.wait()
    to_low[AUX_X] = stage_solid[0].astype(jnp.float32)
    to_high[AUX_X] = stage_solid[span_x - 1].astype(jnp.float32)
    for copy in copies[len(first) :]:
        copy.wait()


def pack_y_rows(pops, from_low, from_high, own_aux, aux_far, to_low, to_high, rows_of):
    span_x, span_y = pops.shape[1], pops.shape[2]
    sides = ((from_low, 1), (from_high, -1))
    for out, sign in ((to_low, -1), (to_high, 1)):
        slots = {k: slot for slot, k in enumerate(moving(1, sign))}
        terms = []
        for number, (k, far) in enumerate(reached(1, sign)):
            sent = far == 1 and k in slots
            rows = pl.ds(far - 1 if sign < 0 else span_y - far, 1)
            plane = out.at[slots[k]] if sent else rows_of.at[number]
            for layer in range(span_x):
                plane[pl.ds(layer + 2, 1)] = pops[k, layer, rows]
            for source, sign_x in sides:
                near = 1 if sign_x > 0 else span_x + 2
                if k in moving(0, sign_x):
                    plane[pl.ds(near, 1)] = source[moving(0, sign_x).index(k), rows]
                if sent:
                    for slot, (other, dist, sign_y) in enumerate(corner_rows(sign_x)):
                        if other == k and sign_y == sign:
                            x = near if dist == 1 else near - sign_x
                            plane[pl.ds(x, 1)] = source[CORNERS, pl.ds(slot, 1)]
            if not sent:
                terms.append((k, plane))
        reads = []
        for k, plane in terms:
            value = plane[...]
            if shifts[k][0] != 0:
                value = pltpu.roll(value, shifts[k][0] % value.shape[0], 0)
            reads.append((k, shift_depth(value, shifts[k][2])))
        for part, value in enumerate(gather_sums(reads)):
            out[N_MOVING + part] = value
        for far in range(1, aux_far + 1):
            rows = pl.ds(far - 1 if sign < 0 else span_y - far, 1)
            slot = AUX_Y + far - 1
            for layer in range(span_x):
                out[slot, pl.ds(layer + 2, 1)] = own_aux[layer, rows].astype(jnp.float32)
            for dist in range(1, aux_far + 1):
                out[slot, pl.ds(2 - dist, 1)] = from_low[AUX_X + dist - 1, rows]
                out[slot, pl.ds(span_x + 1 + dist, 1)] = from_high[AUX_X + dist - 1, rows]


def pack_y_first(pops, obstacle, from_low, from_high, to_low, to_high, rows_of):
    pack_y_rows(pops, from_low, from_high, obstacle, 1, to_low, to_high, rows_of)


def stashed(plane):
    return jnp.max(jnp.where(first_lane(plane.shape), plane, 0.0))


def pack_y_second(pops, lift, peak, others, from_low, from_high, to_low, to_high, row_peak, rows_of):
    pack_y_rows(pops, from_low, from_high, lift, 2, to_low, to_high, rows_of)
    largest = jnp.maximum(jnp.max(peak[...]), jnp.max(others[...]))
    largest = jnp.maximum(largest, stashed(from_low[AUX_X]))
    largest = jnp.maximum(largest, stashed(from_high[AUX_X]))
    row_peak[...] = jnp.full(row_peak.shape, largest, jnp.float32)
    for out in (to_low, to_high):
        plane = out[AUX_Y]
        out[AUX_Y] = jnp.where(first_lane(plane.shape), largest, plane)


def widen(place, wide, sums, pops, x_low, x_high, y_low, y_high, lift):
    span_x, span_y = pops.shape[1], pops.shape[2]
    at_low, at_high = place[0] == 0, place[0] == place[1] - 1
    own = pl.ds(LEAD, span_y)

    def with_lift(k, value, extra):
        if extra is None or shifts[k][2] == 0:
            return value
        return value + lift_coef(k) * extra

    for layer in range(span_x):
        extra = lift("own", layer)
        for k in range(19):
            wide[k, layer + 2, own] = with_lift(k, pops[k, layer], extra)
    sums[...] = jnp.zeros(sums.shape, jnp.float32)
    blank = jnp.zeros((span_y, pops.shape[3]), jnp.float32)
    for name, ref, sign in (("x_low", x_low, 1), ("x_high", x_high, -1)):
        extras = {far: lift(name, far) for far in (1, 2)}
        for k, far in reached(0, sign):
            layer = 2 - far if sign > 0 else span_x + 1 + far
            sent = far == 1 and k in moving(0, sign)
            value = ref[moving(0, sign).index(k)] if sent else blank
            wide[k, layer, own] = with_lift(k, value, extras[far])
        for part in range(N_SUMS):
            sums[part, 0 if sign > 0 else span_x + 1, own] = ref[N_MOVING + part]
    blank = jnp.zeros((span_x + 4, pops.shape[3]), jnp.float32)
    for name, ref, sign, wall in (("y_low", y_low, 1, at_low), ("y_high", y_high, -1, at_high)):
        extras = {far: lift(name, far) for far in (1, 2)}
        for k, far in reached(1, sign):
            row = LEAD - far if sign > 0 else LEAD + span_y - 1 + far
            sent = far == 1 and k in moving(1, sign)
            value = with_lift(k, ref[moving(1, sign).index(k)] if sent else blank, extras[far])
            if sent or shifts[k][2] != 0:
                value = jnp.where(wall, 0.0, value)
            for layer in range(span_x + 4):
                wide[k, layer, pl.ds(row, 1)] = value[layer : layer + 1]
        row = LEAD - 1 if sign > 0 else LEAD + span_y
        for part in range(N_SUMS):
            for layer in range(span_x):
                sums[part, layer + 1, pl.ds(row, 1)] = ref[N_MOVING + part, pl.ds(layer + 2, 1)]


def flow(place, wide, sums, flags, speed):
    span_x, depth = wide.shape[1] - 4, wide.shape[3]
    span_y = wide.shape[2] - 2 * LEAD
    count = span_y + 8
    total_y = place[1] * span_y
    shape = (count, depth)
    grid_y = place[0] * span_y - 1 + lax.broadcasted_iota(jnp.int32, shape, 0)
    grid_z = lax.broadcasted_iota(jnp.int32, shape, 1)
    wall = (grid_y <= 0) | (grid_y >= total_y - 1) | (grid_z == 0) | (grid_z == depth - 1)
    for layer in range(-1, span_x + 1):
        rows = pl.ds(LEAD - 1, count)
        density, *momentum = [sums[part, layer + 1, rows] for part in range(N_SUMS)]
        for k in range(19):
            c_x, c_y, c_z = shifts[k]
            read = shift_depth(wide[k, layer + 2 - c_x, pl.ds(LEAD - 1 - c_y, count)], c_z)
            density = density + read
            for part in range(3):
                if shifts[k][part] > 0:
                    momentum[part] = momentum[part] + read
                elif shifts[k][part] < 0:
                    momentum[part] = momentum[part] - read
        solid = wall | (flags[layer + 1, pl.ds(LEAD - 1, count)] > 0.5)
        inverse = 1.0 / jnp.where(solid, 1.0, density)
        for part in range(3):
            speed[part, layer + 1, pl.ds(LEAD - 1, count)] = jnp.where(
                solid, 0.0, momentum[part] * inverse
            )


def largest_speed(speed, span_x, span_y):
    most = None
    for layer in range(span_x):
        u = [speed[part, layer + 1, pl.ds(LEAD, span_y)] for part in range(3)]
        size = u[0] * u[0] + u[1] * u[1] + u[2] * u[2]
        most = size if most is None else jnp.maximum(most, size)
    return jnp.max(most)


def relax_layer(place, wide, flags, speed, layer):
    depth = wide.shape[3]
    span_y = wide.shape[2] - 2 * LEAD
    shape = (span_y, depth)
    own = pl.ds(LEAD, span_y)
    u = [speed[part, layer + 1, own] for part in range(3)]
    diff = []
    for part in range(3):
        diff.append(
            (
                speed[part, layer + 2, own] - speed[part, layer, own],
                speed[part, layer + 1, pl.ds(LEAD + 1, span_y)]
                - speed[part, layer + 1, pl.ds(LEAD - 1, span_y)],
                shift_depth(u[part], -1) - shift_depth(u[part], 1),
            )
        )
    same = diff[0][0] * diff[0][0] + diff[1][1] * diff[1][1] + diff[2][2] * diff[2][2]
    mixed = None
    for a, b in ((0, 1), (0, 2), (1, 2)):
        cross = diff[a][b] + diff[b][a]
        mixed = cross * cross if mixed is None else mixed + cross * cross
    magnitude = jnp.sqrt(0.5 * same + 0.25 * mixed + strain_floor)
    rate = 1.0 / (base_tau + 3.0 * smag_coef * magnitude)
    solid = solid_layer(place, flags, layer, shape)
    read = []
    density = None
    for k in range(19):
        c_x, c_y, c_z = shifts[k]
        value = shift_depth(wide[k, layer + 2 - c_x, pl.ds(LEAD - c_y, span_y)], c_z)
        read.append(value)
        density = value if density is None else density + value
    level = density * (1.0 - 1.5 * (u[0] * u[0] + u[1] * u[1] + u[2] * u[2]))
    fresh = [None] * 19
    keep = 1.0 - rate
    fresh[0] = jnp.where(solid, read[0], read[0] * keep + (lattice_weight[0] * rate) * level)
    for k in range(1, 19, 2):
        project = None
        for part in range(3):
            if shifts[k][part] != 0:
                term = u[part] if shifts[k][part] > 0 else -u[part]
                project = term if project is None else project + term
        even = level + density * (4.5 * project * project)
        odd = density * (3.0 * project)
        scaled = lattice_weight[k] * rate
        fresh[k] = jnp.where(solid, read[k + 1], read[k] * keep + scaled * (even + odd))
        fresh[k + 1] = jnp.where(solid, read[k], read[k + 1] * keep + scaled * (even - odd))
    return fresh, solid


def solid_layer(place, flags, layer, shape):
    span_y, depth = shape
    grid_y = place[0] * span_y + lax.broadcasted_iota(jnp.int32, shape, 0)
    grid_z = lax.broadcasted_iota(jnp.int32, shape, 1)
    wall = (grid_y <= 0) | (grid_y >= place[1] * span_y - 1) | (grid_z == 0) | (grid_z == depth - 1)
    return wall | (flags[layer + 1, pl.ds(LEAD, span_y)] > 0.5)


def step_first(
    place, table, pops, obstacle, heat_level, x_low, x_high, y_low, y_high,
    fresh_out, flags, lift_out, peak, to_low, to_high, wide, speed, sums,
):
    span_x, span_y, depth = pops.shape[1:]
    own = pl.ds(LEAD, span_y)
    for layer in range(span_x):
        flags[layer + 1, own] = obstacle[layer].astype(jnp.float32)
        flags[layer + 1, pl.ds(LEAD - 1, 1)] = y_low[AUX_Y, pl.ds(layer + 2, 1)]
        flags[layer + 1, pl.ds(LEAD + span_y, 1)] = y_high[AUX_Y, pl.ds(layer + 2, 1)]
    flags[0, own] = x_low[AUX_X]
    flags[span_x + 1, own] = x_high[AUX_X]
    widen(place, wide, sums, pops, x_low, x_high, y_low, y_high, lambda name, far: None)
    flow(place, wide, sums, flags, speed)
    most = largest_speed(speed, span_x, span_y)
    peak[...] = jnp.full(peak.shape, most, jnp.float32)
    outs = ((to_low, -1), (to_high, 1))
    for layer in range(span_x):
        fresh, solid = relax_layer(place, wide, flags, speed, layer)
        force = jnp.zeros((span_y, depth), jnp.float32)
        for level_no in range(table.shape[0]):
            force = jnp.where(heat_level[layer] == level_no, table[level_no], force)
        force = jnp.where(solid, 0.0, force)
        lift_out[layer] = force
        for k in range(19):
            fresh_out[k, layer] = fresh[k]
        for out, sign in outs:
            far = layer + 1 if sign < 0 else span_x - layer
            if far <= 2:
                extra = jnp.where(first_lane(force.shape), most, force) if far == 1 else force
                out[AUX_X + far - 1] = extra
    pack_x(fresh_out, to_low, to_high)


def flow_second(
    place, pops, lift, flags, x_low, x_high, y_low, y_high, row_peak, others,
    wide, speed, peak, sums,
):
    span_x, span_y, depth = pops.shape[1:]
    largest = jnp.maximum(jnp.max(row_peak[...]), jnp.max(others[...]))
    largest = jnp.maximum(largest, stashed(y_low[AUX_Y]))
    largest = jnp.maximum(largest, stashed(y_high[AUX_Y]))
    scale = speed_cap / jnp.sqrt(speed_cap * speed_cap + jnp.full((1, depth), largest, jnp.float32))

    planes = {
        "x_low": (x_low, AUX_X),
        "x_high": (x_high, AUX_X),
        "y_low": (y_low, AUX_Y),
        "y_high": (y_high, AUX_Y),
    }

    def scaled(name, far):
        if name == "own":
            return scale * lift[far]
        ref, first = planes[name]
        plane = ref[first + far - 1]
        return scale * jnp.where(first_lane(plane.shape), 0.0, plane)

    widen(place, wide, sums, pops, x_low, x_high, y_low, y_high, scaled)
    flow(place, wide, sums, flags, speed)
    peak[...] = jnp.full(peak.shape, largest_speed(speed, span_x, span_y), jnp.float32)


def relax_second(place, wide, speed, flags, fresh_out, speed_out):
    span_x, span_y = fresh_out.shape[1], fresh_out.shape[2]
    for layer in range(span_x):
        for part in range(3):
            speed_out[part, layer] = speed[part, layer + 1, pl.ds(LEAD, span_y)]
        fresh, _ = relax_layer(place, wide, flags, speed, layer)
        for k in range(19):
            fresh_out[k, layer] = fresh[k]


def ring(value, axis, hop, closed=True):
    count = lax.axis_size(axis)
    pairs = [(i, i + hop) for i in range(count)]
    if closed:
        pairs = [(i, j % count) for i, j in pairs]
    else:
        pairs = [(i, j) for i, j in pairs if 0 <= j < count]
    return lax.ppermute(value, axis, pairs)


def axis_max(value, axis):
    count = lax.axis_size(axis)
    if count <= 4:
        for other in [ring(value, axis, hop) for hop in range(1, count)]:
            value = jnp.maximum(value, other)
        return value
    window = 1
    while window < count:
        hop = min(window, count - window)
        value = jnp.maximum(value, ring(value, axis, hop))
        window += hop
    return value


def beyond(value, axis):
    count = lax.axis_size(axis)
    if count <= 3:
        return value
    if count == 4:
        return ring(value, axis, 2)
    return axis_max(value, axis)


def shaped(*dims):
    return jax.ShapeDtypeStruct(dims, jnp.float32)


def call(kernel, outs, spaces, scratch=()):
    return pl.pallas_call(
        kernel,
        out_shape=outs,
        in_specs=[pl.BlockSpec(memory_space=space) for space in spaces],
        out_specs=[pl.BlockSpec(memory_space=pltpu.VMEM) for _ in outs],
        scratch_shapes=list(scratch),
        compiler_params=pltpu.CompilerParams(vmem_limit_bytes=40 * 1024 * 1024),
    )


def local(populations, heat_level, obstacle, heat_table):
    _, span_x, span_y, depth = populations.shape
    vmem, smem = pltpu.VMEM, pltpu.SMEM
    place = jnp.stack([lax.axis_index("gy"), lax.axis_size("gy")]).astype(jnp.int32)
    block = shaped(19, span_x, span_y, depth)
    small = shaped(8, depth)
    scratch = (
        pltpu.VMEM((19, span_x + 4, span_y + 2 * LEAD, depth), jnp.float32),
        pltpu.VMEM((3, span_x + 2, span_y + 2 * LEAD, depth), jnp.float32),
        pltpu.VMEM((N_SUMS, span_x + 2, span_y + 2 * LEAD, depth), jnp.float32),
    )
    rows_of = [pltpu.VMEM((len(reached(1, 1)), span_x + 4, depth), jnp.float32)]

    x_face = shaped(AUX_X + 1, span_y, depth)
    y_face = shaped(AUX_Y + 1, span_x + 4, depth)
    to_low, to_high, populations, obstacle = call(
        pack_x_first,
        [x_face, x_face, block, jax.ShapeDtypeStruct(obstacle.shape, obstacle.dtype)],
        [pl.ANY] * 2,
        (
            pltpu.SemaphoreType.DMA((19 * span_x,)),
            pltpu.SemaphoreType.DMA((1,)),
        ),
    )(populations, obstacle)
    x_low, x_high = ring(to_high, "gx", 1), ring(to_low, "gx", -1)
    to_low, to_high = call(pack_y_first, [y_face] * 2, [vmem] * 4, rows_of)(
        populations, obstacle, x_low, x_high
    )
    y_low, y_high = ring(to_high, "gy", 1, False), ring(to_low, "gy", -1, False)

    x_face = shaped(AUX_X + 2, span_y, depth)
    y_face = shaped(AUX_Y + 2, span_x + 4, depth)
    flags = shaped(span_x + 2, span_y + 2 * LEAD, depth)
    current, flags, lift, peak, to_low, to_high = call(
        step_first,
        [block, flags, shaped(span_x, span_y, depth), small, x_face, x_face],
        [smem, smem] + [vmem] * 7,
        scratch,
    )(place, heat_table, populations, obstacle, heat_level, x_low, x_high, y_low, y_high)
    x_low, x_high = ring(to_high, "gx", 1), ring(to_low, "gx", -1)
    others = beyond(peak, "gx")
    to_low, to_high, row_peak = call(pack_y_second, [y_face, y_face, small], [vmem] * 6, rows_of)(
        current, lift, peak, others, x_low, x_high
    )
    y_low, y_high = ring(to_high, "gy", 1), ring(to_low, "gy", -1)
    others = beyond(row_peak, "gy")
    wide, speed, peak = call(
        flow_second,
        [shaped(*scratch[0].shape), shaped(*scratch[1].shape), small],
        [smem] + [vmem] * 9,
        scratch[2:],
    )(place, current, lift, flags, x_low, x_high, y_low, y_high, row_peak, others)
    peak = axis_max(axis_max(peak, "gx"), "gy")[:1]
    current, velocity = call(
        relax_second, [block, shaped(3, span_x, span_y, depth)], [smem] + [vmem] * 3
    )(place, wide, speed, flags)

    force_scale = speed_cap / jnp.sqrt(speed_cap * speed_cap + peak)
    coef = jnp.array([lift_coef(k) for k in range(19)], jnp.float32)
    current = current + coef[:, None, None, None] * (force_scale[None] * lift)[None]
    return (current, velocity)


def solution(mesh):
    return jax.shard_map(
        local,
        mesh=mesh,
        in_specs=(
            P(None, ("member", "gx"), "gy", None),
            P(("member", "gx"), "gy", None),
            P(("member", "gx"), "gy", None),
            P(),
        ),
        out_specs=(P(None, ("member", "gx"), "gy", None), P(None, ("member", "gx"), "gy", None)),
        check_vma=False,
    )
```

```python
import jax
import jax.numpy as jnp
import numpy as np
from jax import lax
from jax.experimental import pallas as pl
from jax.experimental.pallas import tpu as pltpu
from jax.sharding import PartitionSpec as P

STEPS = 2


lattice = np.array(
    [
        [0, 0, 0],
        [1, 0, 0],
        [-1, 0, 0],
        [0, 1, 0],
        [0, -1, 0],
        [0, 0, 1],
        [0, 0, -1],
        [1, 1, 0],
        [-1, -1, 0],
        [1, -1, 0],
        [-1, 1, 0],
        [1, 0, 1],
        [-1, 0, -1],
        [1, 0, -1],
        [-1, 0, 1],
        [0, 1, 1],
        [0, -1, -1],
        [0, 1, -1],
        [0, -1, 1],
    ]
)
lattice_weight = [1.0 / 3.0] + [1.0 / 18.0] * 6 + [1.0 / 36.0] * 12
opposite = [0, 2, 1, 4, 3, 6, 5, 8, 7, 10, 9, 12, 11, 14, 13, 16, 15, 18, 17]
base_tau = 0.52
smag_coef = 0.04
speed_cap = 0.1
strain_floor = 1e-06


LEAD = 8
shifts = [tuple(int(part) for part in row) for row in lattice]


def moving(dim, sign):
    return [k for k in range(19) if shifts[k][dim] == sign]


def reached(dim, sign):
    resting = [k for k in range(19) if shifts[k][dim] == 0]
    return [(k, 1) for k in moving(dim, sign) + resting] + [(k, 2) for k in moving(dim, sign)]


def corner_rows(sign):
    rows = []
    for sign_y in (1, -1):
        for k in range(19):
            if shifts[k][1] == sign_y and shifts[k][0] == 0:
                rows.append((k, 1, sign_y))
            if shifts[k][1] == sign_y and shifts[k][0] == sign:
                rows.append((k, 2, sign_y))
    return rows


N_MOVING = len(moving(0, 1))
N_SUMS = 4
CORNERS = N_MOVING + N_SUMS
AUX_X = CORNERS + 1
AUX_Y = N_MOVING + N_SUMS


def lift_coef(number):
    return 3.0 * lattice_weight[number] * float(shifts[number][2])


def first_lane(shape):
    return lax.broadcasted_iota(jnp.int32, shape, len(shape) - 1) == 0


def shift_depth(value, step):
    if step == 0:
        return value
    depth = value.shape[-1]
    lane = lax.broadcasted_iota(jnp.int32, value.shape, value.ndim - 1)
    if step > 0:
        return jnp.where(lane == 0, 0.0, pltpu.roll(value, 1, value.ndim - 1))
    return jnp.where(lane == depth - 1, 0.0, pltpu.roll(value, depth - 1, value.ndim - 1))


def gather_sums(terms):
    sums = [None] * N_SUMS
    for k, read in terms:
        for part, factor in enumerate((1,) + shifts[k]):
            if factor != 0:
                value = read if factor > 0 else -read
                sums[part] = value if sums[part] is None else sums[part] + value
    return sums


def shift_rows(value, step):
    if step == 0:
        return value
    count = value.shape[0]
    row = lax.broadcasted_iota(jnp.int32, value.shape, 0)
    if step > 0:
        return jnp.where(row == 0, 0.0, pltpu.roll(value, 1, 0))
    return jnp.where(row == count - 1, 0.0, pltpu.roll(value, count - 1, 0))


def pack_x(state, to_low, to_high):
    span_x, span_y = state.shape[1], state.shape[2]
    for out, sign in ((to_low, -1), (to_high, 1)):
        layers = {far: far - 1 if sign < 0 else span_x - far for far in (1, 2)}
        for slot, k in enumerate(moving(0, sign)):
            out[slot] = state[k, layers[1]]
        terms = []
        for k, far in reached(0, sign):
            if far == 2 or shifts[k][0] == 0:
                value = shift_rows(state[k, layers[far]], shifts[k][1])
                terms.append((k, shift_depth(value, shifts[k][2])))
        for part, value in enumerate(gather_sums(terms)):
            out[N_MOVING + part] = value
        for slot, (k, far, sign_y) in enumerate(corner_rows(sign)):
            row = 0 if sign_y < 0 else span_y - 1
            out[CORNERS, pl.ds(slot, 1)] = state[k, layers[far], pl.ds(row, 1)]


def pack_x_first(pops, obstacle, to_low, to_high):
    pack_x(pops, to_low, to_high)
    to_low[AUX_X] = obstacle[0].astype(jnp.float32)
    to_high[AUX_X] = obstacle[obstacle.shape[0] - 1].astype(jnp.float32)


def pack_y_rows(pops, from_low, from_high, own_aux, aux_far, to_low, to_high, rows_of):
    span_x, span_y = pops.shape[1], pops.shape[2]
    sides = ((from_low, 1), (from_high, -1))
    for out, sign in ((to_low, -1), (to_high, 1)):
        slots = {k: slot for slot, k in enumerate(moving(1, sign))}
        terms = []
        for number, (k, far) in enumerate(reached(1, sign)):
            sent = far == 1 and k in slots
            rows = pl.ds(far - 1 if sign < 0 else span_y - far, 1)
            plane = out.at[slots[k]] if sent else rows_of.at[number]
            for layer in range(span_x):
                plane[pl.ds(layer + 2, 1)] = pops[k, layer, rows]
            for source, sign_x in sides:
                near = 1 if sign_x > 0 else span_x + 2
                if k in moving(0, sign_x):
                    plane[pl.ds(near, 1)] = source[moving(0, sign_x).index(k), rows]
                if sent:
                    for slot, (other, dist, sign_y) in enumerate(corner_rows(sign_x)):
                        if other == k and sign_y == sign:
                            x = near if dist == 1 else near - sign_x
                            plane[pl.ds(x, 1)] = source[CORNERS, pl.ds(slot, 1)]
            if not sent:
                terms.append((k, plane))
        reads = []
        for k, plane in terms:
            value = plane[...]
            if shifts[k][0] != 0:
                value = pltpu.roll(value, shifts[k][0] % value.shape[0], 0)
            reads.append((k, shift_depth(value, shifts[k][2])))
        for part, value in enumerate(gather_sums(reads)):
            out[N_MOVING + part] = value
        for far in range(1, aux_far + 1):
            rows = pl.ds(far - 1 if sign < 0 else span_y - far, 1)
            slot = AUX_Y + far - 1
            for layer in range(span_x):
                out[slot, pl.ds(layer + 2, 1)] = own_aux[layer, rows].astype(jnp.float32)
            for dist in range(1, aux_far + 1):
                out[slot, pl.ds(2 - dist, 1)] = from_low[AUX_X + dist - 1, rows]
                out[slot, pl.ds(span_x + 1 + dist, 1)] = from_high[AUX_X + dist - 1, rows]


def pack_y_first(pops, obstacle, from_low, from_high, to_low, to_high, rows_of):
    pack_y_rows(pops, from_low, from_high, obstacle, 1, to_low, to_high, rows_of)


def stashed(plane):
    return jnp.max(jnp.where(first_lane(plane.shape), plane, 0.0))


def pack_y_second(pops, lift, peak, others, from_low, from_high, to_low, to_high, row_peak, rows_of):
    pack_y_rows(pops, from_low, from_high, lift, 2, to_low, to_high, rows_of)
    largest = jnp.maximum(jnp.max(peak[...]), jnp.max(others[...]))
    largest = jnp.maximum(largest, stashed(from_low[AUX_X]))
    largest = jnp.maximum(largest, stashed(from_high[AUX_X]))
    row_peak[...] = jnp.full(row_peak.shape, largest, jnp.float32)
    for out in (to_low, to_high):
        plane = out[AUX_Y]
        out[AUX_Y] = jnp.where(first_lane(plane.shape), largest, plane)


def widen(place, wide, sums, pops, x_low, x_high, y_low, y_high, lift):
    span_x, span_y = pops.shape[1], pops.shape[2]
    at_low, at_high = place[0] == 0, place[0] == place[1] - 1
    own = pl.ds(LEAD, span_y)

    def with_lift(k, value, extra):
        if extra is None or shifts[k][2] == 0:
            return value
        return value + lift_coef(k) * extra

    for layer in range(span_x):
        extra = lift("own", layer)
        for k in range(19):
            wide[k, layer + 2, own] = with_lift(k, pops[k, layer], extra)
    sums[...] = jnp.zeros(sums.shape, jnp.float32)
    blank = jnp.zeros((span_y, pops.shape[3]), jnp.float32)
    for name, ref, sign in (("x_low", x_low, 1), ("x_high", x_high, -1)):
        extras = {far: lift(name, far) for far in (1, 2)}
        for k, far in reached(0, sign):
            layer = 2 - far if sign > 0 else span_x + 1 + far
            sent = far == 1 and k in moving(0, sign)
            value = ref[moving(0, sign).index(k)] if sent else blank
            wide[k, layer, own] = with_lift(k, value, extras[far])
        for part in range(N_SUMS):
            sums[part, 0 if sign > 0 else span_x + 1, own] = ref[N_MOVING + part]
    blank = jnp.zeros((span_x + 4, pops.shape[3]), jnp.float32)
    for name, ref, sign, wall in (("y_low", y_low, 1, at_low), ("y_high", y_high, -1, at_high)):
        extras = {far: lift(name, far) for far in (1, 2)}
        for k, far in reached(1, sign):
            row = LEAD - far if sign > 0 else LEAD + span_y - 1 + far
            sent = far == 1 and k in moving(1, sign)
            value = with_lift(k, ref[moving(1, sign).index(k)] if sent else blank, extras[far])
            if sent or shifts[k][2] != 0:
                value = jnp.where(wall, 0.0, value)
            for layer in range(span_x + 4):
                wide[k, layer, pl.ds(row, 1)] = value[layer : layer + 1]
        row = LEAD - 1 if sign > 0 else LEAD + span_y
        for part in range(N_SUMS):
            for layer in range(span_x):
                sums[part, layer + 1, pl.ds(row, 1)] = ref[N_MOVING + part, pl.ds(layer + 2, 1)]


def flow(place, wide, sums, flags, speed):
    span_x, depth = wide.shape[1] - 4, wide.shape[3]
    span_y = wide.shape[2] - 2 * LEAD
    count = span_y + 8
    total_y = place[1] * span_y
    shape = (count, depth)
    grid_y = place[0] * span_y - 1 + lax.broadcasted_iota(jnp.int32, shape, 0)
    grid_z = lax.broadcasted_iota(jnp.int32, shape, 1)
    wall = (grid_y <= 0) | (grid_y >= total_y - 1) | (grid_z == 0) | (grid_z == depth - 1)
    for layer in range(-1, span_x + 1):
        rows = pl.ds(LEAD - 1, count)
        density, *momentum = [sums[part, layer + 1, rows] for part in range(N_SUMS)]
        for k in range(19):
            c_x, c_y, c_z = shifts[k]
            read = shift_depth(wide[k, layer + 2 - c_x, pl.ds(LEAD - 1 - c_y, count)], c_z)
            density = density + read
            for part in range(3):
                if shifts[k][part] > 0:
                    momentum[part] = momentum[part] + read
                elif shifts[k][part] < 0:
                    momentum[part] = momentum[part] - read
        solid = wall | (flags[layer + 1, pl.ds(LEAD - 1, count)] > 0.5)
        inverse = 1.0 / jnp.where(solid, 1.0, density)
        for part in range(3):
            speed[part, layer + 1, pl.ds(LEAD - 1, count)] = jnp.where(
                solid, 0.0, momentum[part] * inverse
            )


def largest_speed(speed, span_x, span_y):
    most = None
    for layer in range(span_x):
        u = [speed[part, layer + 1, pl.ds(LEAD, span_y)] for part in range(3)]
        size = u[0] * u[0] + u[1] * u[1] + u[2] * u[2]
        most = size if most is None else jnp.maximum(most, size)
    return jnp.max(most)


def relax_layer(place, wide, flags, speed, layer):
    depth = wide.shape[3]
    span_y = wide.shape[2] - 2 * LEAD
    shape = (span_y, depth)
    own = pl.ds(LEAD, span_y)
    u = [speed[part, layer + 1, own] for part in range(3)]
    diff = []
    for part in range(3):
        diff.append(
            (
                speed[part, layer + 2, own] - speed[part, layer, own],
                speed[part, layer + 1, pl.ds(LEAD + 1, span_y)]
                - speed[part, layer + 1, pl.ds(LEAD - 1, span_y)],
                shift_depth(u[part], -1) - shift_depth(u[part], 1),
            )
        )
    same = diff[0][0] * diff[0][0] + diff[1][1] * diff[1][1] + diff[2][2] * diff[2][2]
    mixed = None
    for a, b in ((0, 1), (0, 2), (1, 2)):
        cross = diff[a][b] + diff[b][a]
        mixed = cross * cross if mixed is None else mixed + cross * cross
    magnitude = jnp.sqrt(0.5 * same + 0.25 * mixed + strain_floor)
    rate = 1.0 / (base_tau + 3.0 * smag_coef * magnitude)
    solid = solid_layer(place, flags, layer, shape)
    read = []
    density = None
    for k in range(19):
        c_x, c_y, c_z = shifts[k]
        value = shift_depth(wide[k, layer + 2 - c_x, pl.ds(LEAD - c_y, span_y)], c_z)
        read.append(value)
        density = value if density is None else density + value
    level = density * (1.0 - 1.5 * (u[0] * u[0] + u[1] * u[1] + u[2] * u[2]))
    fresh = [None] * 19
    keep = 1.0 - rate
    fresh[0] = jnp.where(solid, read[0], read[0] * keep + (lattice_weight[0] * rate) * level)
    for k in range(1, 19, 2):
        project = None
        for part in range(3):
            if shifts[k][part] != 0:
                term = u[part] if shifts[k][part] > 0 else -u[part]
                project = term if project is None else project + term
        even = level + density * (4.5 * project * project)
        odd = density * (3.0 * project)
        scaled = lattice_weight[k] * rate
        fresh[k] = jnp.where(solid, read[k + 1], read[k] * keep + scaled * (even + odd))
        fresh[k + 1] = jnp.where(solid, read[k], read[k + 1] * keep + scaled * (even - odd))
    return fresh, solid


def solid_layer(place, flags, layer, shape):
    span_y, depth = shape
    grid_y = place[0] * span_y + lax.broadcasted_iota(jnp.int32, shape, 0)
    grid_z = lax.broadcasted_iota(jnp.int32, shape, 1)
    wall = (grid_y <= 0) | (grid_y >= place[1] * span_y - 1) | (grid_z == 0) | (grid_z == depth - 1)
    return wall | (flags[layer + 1, pl.ds(LEAD, span_y)] > 0.5)


def step_first(
    place, table, pops, obstacle, heat_level, x_low, x_high, y_low, y_high,
    fresh_out, flags, lift_out, peak, to_low, to_high, wide, speed, sums,
):
    span_x, span_y, depth = pops.shape[1:]
    own = pl.ds(LEAD, span_y)
    for layer in range(span_x):
        flags[layer + 1, own] = obstacle[layer].astype(jnp.float32)
        flags[layer + 1, pl.ds(LEAD - 1, 1)] = y_low[AUX_Y, pl.ds(layer + 2, 1)]
        flags[layer + 1, pl.ds(LEAD + span_y, 1)] = y_high[AUX_Y, pl.ds(layer + 2, 1)]
    flags[0, own] = x_low[AUX_X]
    flags[span_x + 1, own] = x_high[AUX_X]
    widen(place, wide, sums, pops, x_low, x_high, y_low, y_high, lambda name, far: None)
    flow(place, wide, sums, flags, speed)
    most = largest_speed(speed, span_x, span_y)
    peak[...] = jnp.full(peak.shape, most, jnp.float32)
    outs = ((to_low, -1), (to_high, 1))
    for layer in range(span_x):
        fresh, solid = relax_layer(place, wide, flags, speed, layer)
        force = jnp.zeros((span_y, depth), jnp.float32)
        for level_no in range(table.shape[0]):
            force = jnp.where(heat_level[layer] == level_no, table[level_no], force)
        force = jnp.where(solid, 0.0, force)
        lift_out[layer] = force
        for k in range(19):
            fresh_out[k, layer] = fresh[k]
        for out, sign in outs:
            far = layer + 1 if sign < 0 else span_x - layer
            if far <= 2:
                extra = jnp.where(first_lane(force.shape), most, force) if far == 1 else force
                out[AUX_X + far - 1] = extra
    pack_x(fresh_out, to_low, to_high)


def flow_second(
    place, pops, lift, flags, x_low, x_high, y_low, y_high, row_peak, others,
    wide, speed, peak, sums,
):
    span_x, span_y, depth = pops.shape[1:]
    largest = jnp.maximum(jnp.max(row_peak[...]), jnp.max(others[...]))
    largest = jnp.maximum(largest, stashed(y_low[AUX_Y]))
    largest = jnp.maximum(largest, stashed(y_high[AUX_Y]))
    scale = speed_cap / jnp.sqrt(speed_cap * speed_cap + jnp.full((1, depth), largest, jnp.float32))

    planes = {
        "x_low": (x_low, AUX_X),
        "x_high": (x_high, AUX_X),
        "y_low": (y_low, AUX_Y),
        "y_high": (y_high, AUX_Y),
    }

    def scaled(name, far):
        if name == "own":
            return scale * lift[far]
        ref, first = planes[name]
        plane = ref[first + far - 1]
        return scale * jnp.where(first_lane(plane.shape), 0.0, plane)

    widen(place, wide, sums, pops, x_low, x_high, y_low, y_high, scaled)
    flow(place, wide, sums, flags, speed)
    peak[...] = jnp.full(peak.shape, largest_speed(speed, span_x, span_y), jnp.float32)


def relax_second(place, wide, speed, flags, fresh_out, speed_out):
    span_x, span_y = fresh_out.shape[1], fresh_out.shape[2]
    for layer in range(span_x):
        for part in range(3):
            speed_out[part, layer] = speed[part, layer + 1, pl.ds(LEAD, span_y)]
        fresh, _ = relax_layer(place, wide, flags, speed, layer)
        for k in range(19):
            fresh_out[k, layer] = fresh[k]


def ring(value, axis, hop, closed=True):
    count = lax.axis_size(axis)
    pairs = [(i, i + hop) for i in range(count)]
    if closed:
        pairs = [(i, j % count) for i, j in pairs]
    else:
        pairs = [(i, j) for i, j in pairs if 0 <= j < count]
    return lax.ppermute(value, axis, pairs)


def axis_max(value, axis):
    count = lax.axis_size(axis)
    if count <= 4:
        for other in [ring(value, axis, hop) for hop in range(1, count)]:
            value = jnp.maximum(value, other)
        return value
    window = 1
    while window < count:
        hop = min(window, count - window)
        value = jnp.maximum(value, ring(value, axis, hop))
        window += hop
    return value


def beyond(value, axis):
    count = lax.axis_size(axis)
    if count <= 3:
        return value
    if count == 4:
        return ring(value, axis, 2)
    return axis_max(value, axis)


def shaped(*dims):
    return jax.ShapeDtypeStruct(dims, jnp.float32)


def call(kernel, outs, spaces, scratch=()):
    return pl.pallas_call(
        kernel,
        out_shape=outs,
        in_specs=[pl.BlockSpec(memory_space=space) for space in spaces],
        out_specs=[pl.BlockSpec(memory_space=pltpu.VMEM) for _ in outs],
        scratch_shapes=list(scratch),
        compiler_params=pltpu.CompilerParams(vmem_limit_bytes=40 * 1024 * 1024),
    )


def local(populations, heat_level, obstacle, heat_table):
    _, span_x, span_y, depth = populations.shape
    vmem, smem = pltpu.VMEM, pltpu.SMEM
    place = jnp.stack([lax.axis_index("gy"), lax.axis_size("gy")]).astype(jnp.int32)
    block = shaped(19, span_x, span_y, depth)
    small = shaped(8, depth)
    scratch = (
        pltpu.VMEM((19, span_x + 4, span_y + 2 * LEAD, depth), jnp.float32),
        pltpu.VMEM((3, span_x + 2, span_y + 2 * LEAD, depth), jnp.float32),
        pltpu.VMEM((N_SUMS, span_x + 2, span_y + 2 * LEAD, depth), jnp.float32),
    )
    rows_of = [pltpu.VMEM((len(reached(1, 1)), span_x + 4, depth), jnp.float32)]

    x_face = shaped(AUX_X + 1, span_y, depth)
    y_face = shaped(AUX_Y + 1, span_x + 4, depth)
    to_low, to_high = call(pack_x_first, [x_face] * 2, [vmem] * 2)(populations, obstacle)
    x_low, x_high = ring(to_high, "gx", 1), ring(to_low, "gx", -1)
    to_low, to_high = call(pack_y_first, [y_face] * 2, [vmem] * 4, rows_of)(
        populations, obstacle, x_low, x_high
    )
    y_low, y_high = ring(to_high, "gy", 1, False), ring(to_low, "gy", -1, False)

    x_face = shaped(AUX_X + 2, span_y, depth)
    y_face = shaped(AUX_Y + 2, span_x + 4, depth)
    flags = shaped(span_x + 2, span_y + 2 * LEAD, depth)
    current, flags, lift, peak, to_low, to_high = call(
        step_first,
        [block, flags, shaped(span_x, span_y, depth), small, x_face, x_face],
        [smem, smem] + [vmem] * 7,
        scratch,
    )(place, heat_table, populations, obstacle, heat_level, x_low, x_high, y_low, y_high)
    x_low, x_high = ring(to_high, "gx", 1), ring(to_low, "gx", -1)
    others = beyond(peak, "gx")
    to_low, to_high, row_peak = call(pack_y_second, [y_face, y_face, small], [vmem] * 6, rows_of)(
        current, lift, peak, others, x_low, x_high
    )
    y_low, y_high = ring(to_high, "gy", 1), ring(to_low, "gy", -1)
    others = beyond(row_peak, "gy")
    wide, speed, peak = call(
        flow_second,
        [shaped(*scratch[0].shape), shaped(*scratch[1].shape), small],
        [smem] + [vmem] * 9,
        scratch[2:],
    )(place, current, lift, flags, x_low, x_high, y_low, y_high, row_peak, others)
    peak = axis_max(axis_max(peak, "gx"), "gy")[:1]
    current, velocity = call(
        relax_second, [block, shaped(3, span_x, span_y, depth)], [smem] + [vmem] * 3
    )(place, wide, speed, flags)

    force_scale = speed_cap / jnp.sqrt(speed_cap * speed_cap + peak)
    coef = jnp.array([lift_coef(k) for k in range(19)], jnp.float32)
    current = current + coef[:, None, None, None] * (force_scale[None] * lift)[None]
    return (current, velocity)


def solution(mesh):
    return jax.shard_map(
        local,
        mesh=mesh,
        in_specs=(
            P(None, ("member", "gx"), "gy", None),
            P(("member", "gx"), "gy", None),
            P(("member", "gx"), "gy", None),
            P(),
        ),
        out_specs=(P(None, ("member", "gx"), "gy", None), P(None, ("member", "gx"), "gy", None)),
        check_vma=False,
    )
```
